16 devices in a mesh: rep: 2 (over y, z), dp: 8 (over x, core).
Axes of the slice: x: 4, y: 2, z: 1, core: 2. Of those that a mesh axis runs over, the one named last changes fastest.
The devices are a block of a 4x4x8 slice.
Arguments:
- g_w_gate: bfloat16 [16, 2, 1024, 3328], P(('rep', 'dp')), parts along dimension 0
- g_w_up: bfloat16 [16, 2, 1024, 3328], P(('rep', 'dp')), parts along dimension 0
- g_w_down: bfloat16 [16, 2, 3328, 1024], P(('rep', 'dp')), parts along dimension 0
- w_gate: bfloat16 [2, 1024, 3328], replicated
- w_up: bfloat16 [2, 1024, 3328], replicated
- w_down: bfloat16 [2, 3328, 1024], replicated
- m_w_gate: float32 [2, 1024, 3328], P(None, 'dp')
- m_w_up: float32 [2, 1024, 3328], P(None, 'dp')
- m_w_down: float32 [2, 3328, 1024], P(None, 'dp')
- v_w_gate: float32 [2, 1024, 3328], P(None, 'dp')
- v_w_up: float32 [2, 1024, 3328], P(None, 'dp')
- v_w_down: float32 [2, 3328, 1024], P(None, 'dp')
Outputs:
- output 1: bfloat16 [4, 1024, 3328], P('rep'), parts along dimension 0
- output 2: bfloat16 [4, 1024, 3328], P('rep'), parts along dimension 0
- output 3: bfloat16 [4, 3328, 1024], P('rep'), parts along dimension 0
- output 4: float32 [4, 1024, 3328], P('rep', 'dp'), parts along dimension 0
- output 5: float32 [4, 1024, 3328], P('rep', 'dp'), parts along dimension 0
- output 6: float32 [4, 3328, 1024], P('rep', 'dp'), parts along dimension 0
- output 7: float32 [4, 1024, 3328], P('rep', 'dp'), parts along dimension 0
- output 8: float32 [4, 1024, 3328], P('rep', 'dp'), parts along dimension 0
- output 9: float32 [4, 3328, 1024], P('rep', 'dp'), parts along dimension 0
There are 2 independent parts. The reference program is written for one: setup_inputs(seed, part) draws one part's arguments, and reference() takes and returns one part's arrays. A program takes and returns all parts, laid end to end along the dimension named above; an argument that names none is the same for every part.
All inputs are finite; a program needn't handle non-finite values.
Results may differ from the reference program's by a relative error of at most 0.022.
Values are sent between devices in bfloat16 or wider.
A program may use at most 768 MiB of HBM per device.

```python
import jax
import jax.numpy as jnp
from jax import lax

DEVICES = 8
D = 1024
FF = 3328
LAYERS = 2
NAMES = ("w_gate", "w_up", "w_down")
SHAPES = {"w_gate": (LAYERS, D, FF), "w_up": (LAYERS, D, FF), "w_down": (LAYERS, FF, D)}


def setup_inputs(seed: int = 0, part: int = 0) -> dict:
    kz, *keys = jax.random.split(jax.random.key(seed), 1 + 5 * len(NAMES))
    loud = 2.0 ** jax.random.uniform(kz, (), jnp.float32, -1.0, 1.0)
    drawn = {}
    for name, key, both in zip(NAMES, keys[:3], keys[3:6], strict=True):
        own = jax.random.normal(jax.random.fold_in(key, part), (DEVICES, *SHAPES[name]), jnp.float32)
        shared = jax.random.normal(jax.random.fold_in(both, part), SHAPES[name], jnp.float32)
        drawn["g_" + name] = (loud * (0.7 * shared / DEVICES + 0.7 * own * DEVICES**-0.5)).astype(jnp.bfloat16)
    for name, key in zip(NAMES, keys[6:9], strict=True):
        drawn[name] = (jax.random.normal(key, SHAPES[name], jnp.float32) * SHAPES[name][1] ** -0.5).astype(jnp.bfloat16)
    for name, key in zip(NAMES, keys[9:12], strict=True):
        drawn["m_" + name] = loud * 0.5 * jax.random.normal(key, SHAPES[name], jnp.float32)
    for name, key in zip(NAMES, keys[12:15], strict=True):
        drawn["v_" + name] = loud * loud * jax.random.uniform(key, SHAPES[name], jnp.float32, 0.5, 1.5)
    return drawn


def adamw(w, m, v, g):
    m = 0.9 * m + 0.1 * g
    v = 0.95 * v + 0.05 * g * g
    step = m * lax.rsqrt(v + 1e-8) + 0.1 * w
    return (w - 0.02 * step).astype(jnp.bfloat16), m, v


def reference(g_w_gate, g_w_up, g_w_down, w_gate, w_up, w_down, m_w_gate, m_w_up, m_w_down, v_w_gate, v_w_up, v_w_down):
    def total(terms):
        return lax.scan(lambda so_far, term: (so_far + term.astype(jnp.float32), None), jnp.zeros(terms.shape[1:], jnp.float32), terms)[0]

    gradients = [total(terms).astype(jnp.bfloat16).astype(jnp.float32) for terms in (g_w_gate, g_w_up, g_w_down)]
    new = [
        adamw(w.astype(jnp.float32), m, v, g)
        for w, m, v, g in zip((w_gate, w_up, w_down), (m_w_gate, m_w_up, m_w_down), (v_w_gate, v_w_up, v_w_down), gradients, strict=True)
    ]
    return tuple(one[which] for which in range(3) for one in new)
```

```python
import functools

import jax
import jax.numpy as jnp
from jax import lax
from jax.experimental import pallas as pl
from jax.experimental.pallas import tpu as pltpu
from jax.sharding import PartitionSpec as P

MESH = pl.DeviceIdType.MESH
CORES = 2
STRIP = 16
SLOTS = 6
SETS = 3


def f32(x):
    return x.astype(jnp.float32)


def strips(rows, body):
    def one(i, carry):
        body(pl.ds(pl.multiple_of(i * STRIP, STRIP), STRIP))
        return carry

    lax.fori_loop(0, rows // STRIP, one, None)


def kernel(chips, layers, kinds, *refs):
    count = len(kinds)
    take = iter(refs)
    g, w, m, v, w_out, m_out, v_out, part, arrived = ([next(take) for _ in range(count)] for _ in range(9))
    shapes = max(kinds) + 1
    own, m_set, v_set, w_set = ([next(take) for _ in range(shapes)] for _ in range(4))
    own_sem, set_in, set_out, pair_send, pair_recv, ring_send, ring_recv, gather_send, gather_recv, local_sem = take

    me = lax.axis_index("dp")
    chip, core = me // CORES, me % CORES
    partner = chip * CORES + (1 - core)
    turn = [lax.rem(chip + d, chips) for d in range(chips)]
    right, left = turn[1] * CORES + core, turn[chips - 1] * CORES + core
    far = chips // 2

    chunks = [(a, layer) for a in range(count) for layer in range(layers)]
    rows = [r.shape[2] for r in part]
    half = [r // 2 for r in rows]

    barrier = pltpu.get_barrier_semaphore()
    for other in (partner, right, left):
        pl.semaphore_signal(barrier, inc=1, device_id={"dp": other}, device_id_type=MESH)
    pl.semaphore_wait(barrier, 3)

    def remote(src, dst, send, recv, to):
        return pltpu.make_async_remote_copy(src_ref=src, dst_ref=dst, send_sem=send, recv_sem=recv, device_id={"dp": to}, device_id_type=MESH)

    waits = []

    order = (far, 1, chips - 1, 0)

    def pair_copy(j, n):
        a, layer = chunks[j]
        d = order[n]
        src = g[a].at[0, layer, pl.ds(pl.multiple_of((turn[d] * CORES + 1 - core) * rows[a], STRIP), rows[a])]
        s = j * chips + n
        return remote(src, part[a].at[layer, d], pair_send.at[s], pair_recv.at[s], partner)

    def start_pair(j):
        for n in range(chips):
            copy = pair_copy(j, n)
            copy.start()
            waits.append(copy.wait_send)

    seen = set()

    def need_pair(j, d):
        if (j, d) not in seen:
            seen.add((j, d))
            pair_copy(j, order.index(d)).wait_recv()

    uses = []
    for s in range(len(chunks) + 2):
        if s < len(chunks):
            uses += [(s, far, 0), (s, far, 1), (s, 1, 1), (s, chips - 1, 0)]
        if 0 <= s - 1 < len(chunks):
            uses += [(s - 1, 1, 0), (s - 1, chips - 1, 1)]
        if 0 <= s - 2 < len(chunks):
            uses += [(s - 2, 0, 0), (s - 2, 0, 1)]
    of_kind = [[u for u in uses if kinds[chunks[u[0]][0]] == q] for q in range(shapes)]

    def own_copy(q, i):
        j, d, h = of_kind[q][i]
        a, layer = chunks[j]
        src = g[a].at[0, layer, pl.ds(pl.multiple_of((turn[d] * CORES + core) * rows[a] + h * half[a], STRIP), half[a])]
        return pltpu.make_async_copy(src, own[q].at[i % SLOTS], own_sem.at[q, i % SLOTS])

    for q in range(shapes):
        for i in range(min(SLOTS, len(of_kind[q]))):
            own_copy(q, i).start()
    used = [0] * shapes

    def add_own(j, d, h, extra, finish=None):
        a, layer = chunks[j]
        q = kinds[a]
        i = used[q]
        used[q] += 1
        assert of_kind[q][i] == (j, d, h)
        need_pair(j, d)
        own_copy(q, i).wait()
        mine = own[q].at[i % SLOTS]
        total = part[a].at[layer, d, pl.ds(h * half[a], half[a])]

        def body(strip):
            x = f32(total[strip, :]) + f32(mine[strip, :])
            for one in extra:
                x = x + f32(one[strip, :])
            x = x.astype(jnp.bfloat16)
            total[strip, :] = x if finish is None else finish(strip, f32(x))

        strips(half[a], body)
        if i + SLOTS < len(of_kind[q]):
            own_copy(q, i + SLOTS).start()
        return total

    def ring_copy(j, slot):
        a, layer = chunks[j]
        d, h = ((far, 0), (1, 1), (1, 0), (far, 1), (chips - 1, 0), (chips - 1, 1))[slot]
        src = part[a].at[layer, d, pl.ds(h * half[a], half[a])]
        s = j * 6 + slot
        return remote(src, arrived[a].at[layer, slot], ring_send.at[s], ring_recv.at[s], right if slot < 3 else left)

    def send(j, slot):
        copy = ring_copy(j, slot)
        copy.start()
        waits.append(copy.wait_send)

    def arrival(j, slot):
        ring_copy(j, slot).wait_recv()
        a, layer = chunks[j]
        return arrived[a].at[layer, slot]

    def first(j):
        add_own(j, far, 0, ())
        send(j, 0)
        add_own(j, far, 1, ())
        send(j, 3)
        add_own(j, 1, 1, ())
        send(j, 1)
        add_own(j, chips - 1, 0, ())
        send(j, 4)

    def middle(j):
        add_own(j, 1, 0, (arrival(j, 0),))
        send(j, 2)
        add_own(j, chips - 1, 1, (arrival(j, 3),))
        send(j, 5)

    units = [[(j, h) for j in range(len(chunks)) for h in range(2) if kinds[chunks[j][0]] == q] for q in range(shapes)]

    def set_copies(q, i):
        j, h = units[q][i]
        a, layer = chunks[j]
        cut = pl.ds(h * half[a], half[a])
        mine = pl.ds(pl.multiple_of(me * rows[a] + h * half[a], STRIP), half[a])
        t = i % SETS
        return [
            pltpu.make_async_copy(m[a].at[layer, cut], m_set[q].at[t], set_in.at[q, t, 0]),
            pltpu.make_async_copy(v[a].at[layer, cut], v_set[q].at[t], set_in.at[q, t, 1]),
            pltpu.make_async_copy(w[a].at[layer, mine], w_set[q].at[t], set_in.at[q, t, 2]),
        ], [
            pltpu.make_async_copy(m_set[q].at[t], m_out[a].at[layer, cut], set_out.at[q, t, 0]),
            pltpu.make_async_copy(v_set[q].at[t], v_out[a].at[layer, cut], set_out.at[q, t, 1]),
        ]

    def start_set(q, i):
        if i < len(units[q]):
            if i >= SETS:
                for copy in set_copies(q, i - SETS)[1]:
                    copy.wait()
            for copy in set_copies(q, i)[0]:
                copy.start()

    for q in range(shapes):
        for i in range(SETS - 1):
            start_set(q, i)

    def update(j, h, extra):
        a, layer = chunks[j]
        q = kinds[a]
        i = units[q].index((j, h))
        ins, outs = set_copies(q, i)
        for copy in ins:
            copy.wait()
        mm, vv, ww = (s[q].at[i % SETS] for s in (m_set, v_set, w_set))

        def finish(strip, grad):
            old = f32(ww[strip, :])
            new_m = 0.9 * mm[strip, :] + 0.1 * grad
            new_v = 0.95 * vv[strip, :] + 0.05 * grad * grad
            mm[strip, :] = new_m
            vv[strip, :] = new_v
            step = new_m * lax.rsqrt(new_v + 1e-8) + 0.1 * old
            return (old - 0.02 * step).astype(jnp.bfloat16)

        add_own(j, 0, h, extra, finish)
        for copy in outs:
            copy.start()
        start_set(q, i + SETS - 1)

    def block(a, layer, chip_of, core_of, h=None):
        base = (chip_of * CORES + core_of) * rows[a]
        if h is None:
            return w_out[a].at[layer, pl.ds(pl.multiple_of(base, STRIP), rows[a])]
        return w_out[a].at[layer, pl.ds(pl.multiple_of(base + h * half[a], STRIP), half[a])]

    def gather_copy(j, n):
        a, layer = chunks[j]
        s = (gather_send.at[j, n], gather_recv.at[j, n])
        mine = lambda h: part[a].at[layer, 0, pl.ds(h * half[a], half[a])]
        if n < 4:
            h, to = n % 2, right if n < 2 else left
            return remote(mine(h), block(a, layer, chip, core, h), *s, to)
        if n < 6:
            d, h, to = ((chips - 1, 0, right), (1, 1, left))[n - 4]
            there = block(a, layer, turn[d], core, h)
            return remote(there, there, *s, to)
        if n == 6:
            return remote(part[a].at[layer, 0], block(a, layer, chip, core), *s, partner)
        d, h = ((chips - 1, None), (1, None), (far, 0), (far, 1))[n - 7]
        there = block(a, layer, turn[d], core, h)
        return remote(there, there, *s, partner)

    def go(j, n):
        copy = gather_copy(j, n)
        copy.start()
        waits.append(copy.wait_send)
        if n >= 6:
            waits.append(copy.wait_recv)

    def final(j):
        a, layer = chunks[j]
        update(j, 0, (arrival(j, 2), arrival(j, 4)))
        go(j, 0)
        update(j, 1, (arrival(j, 1), arrival(j, 5)))
        go(j, 3)
        go(j, 1)
        go(j, 2)
        go(j, 6)
        keep = pltpu.make_async_copy(part[a].at[layer, 0], block(a, layer, chip, core), local_sem.at[j])
        keep.start()
        waits.append(keep.wait)

    def pass_on(j):
        gather_copy(j, 0).wait_recv()
        go(j, 4)
        gather_copy(j, 3).wait_recv()
        go(j, 5)
        gather_copy(j, 1).wait_recv()
        go(j, 7)
        gather_copy(j, 2).wait_recv()
        go(j, 8)

    def hand_over(j):
        gather_copy(j, 4).wait_recv()
        go(j, 9)
        gather_copy(j, 5).wait_recv()
        go(j, 10)

    total = len(chunks)
    start_pair(0)
    for s in range(total + 5):
        if s + 1 < total:
            start_pair(s + 1)
        for back, act in ((0, first), (1, middle), (2, final), (4, pass_on), (5, hand_over)):
            if 0 <= s - back < total:
                act(s - back)

    for q in range(shapes):
        for i in range(max(0, len(units[q]) - SETS), len(units[q])):
            for copy in set_copies(q, i)[1]:
                copy.wait()
    for wait in waits:
        wait()


def solution(mesh):
    devices = mesh.shape["dp"]
    chips = devices // CORES

    def step(*arrays):
        terms, weights, m, v = (arrays[i : i + 3] for i in (0, 3, 6, 9))
        count, layers = len(weights), weights[0].shape[0]
        blocks = [one.shape[1:] for one in m]
        distinct = list(dict.fromkeys(blocks))
        kinds = tuple(distinct.index(b) for b in blocks)
        chunks = count * layers
        any_space = pl.BlockSpec(memory_space=pl.ANY)
        bf16 = jnp.bfloat16
        halves = [(b[0] // 2, b[1]) for b in distinct]
        dma = pltpu.SemaphoreType.DMA
        out = pl.pallas_call(
            functools.partial(kernel, chips, layers, kinds),
            out_shape=[jax.ShapeDtypeStruct(one.shape, one.dtype) for one in (*weights, *m, *v)],
            in_specs=[any_space] * 4 * count,
            out_specs=[any_space] * 3 * count,
            scratch_shapes=[pltpu.VMEM((layers, chips, *b), bf16) for b in blocks]
            + [pltpu.VMEM((layers, 6, b[0] // 2, b[1]), bf16) for b in blocks]
            + [pltpu.VMEM((SLOTS, *b), bf16) for b in halves]
            + [pltpu.VMEM((SETS, *b), jnp.float32) for b in halves] * 2
            + [pltpu.VMEM((SETS, *b), bf16) for b in halves]
            + [dma((len(distinct), SLOTS)), dma((len(distinct), SETS, 3)), dma((len(distinct), SETS, 2))]
            + [dma((chunks * chips,))] * 2
            + [dma((chunks * 6,))] * 2
            + [dma((chunks, 11))] * 2
            + [dma((chunks,))],
            compiler_params=pltpu.CompilerParams(collective_id=0, has_side_effects=True, vmem_limit_bytes=62 * 1024 * 1024),
        )(*terms, *weights, *m, *v)
        return tuple(out)

    all_of, cut = P(None, None, None), P(None, "dp", None)
    return jax.shard_map(
        step,
        mesh=mesh,
        in_specs=(P(("rep", "dp"), None, None, None),) * 3 + (all_of,) * 3 + (cut,) * 6,
        out_specs=(P("rep", None, None),) * 3 + (P("rep", "dp", None),) * 6,
        check_vma=False,
    )
```

```python
import functools

import jax
import jax.numpy as jnp
from jax import lax
from jax.experimental import pallas as pl
from jax.experimental.pallas import tpu as pltpu
from jax.sharding import PartitionSpec as P


MESH = pl.DeviceIdType.MESH
CORES = 2
STRIP = 16
SLOTS = 6
VMEM = 67043328
SETS = 3


def f32(x):
    return x.astype(jnp.float32)


def strips(rows, body):
    def one(i, carry):
        body(pl.ds(pl.multiple_of(i * STRIP, STRIP), STRIP))
        return carry

    lax.fori_loop(0, rows // STRIP, one, None)


def kernel(chips, layers, kinds, *refs):
    count = len(kinds)
    last = count - 1
    take = iter(refs)
    g, w, m, v = ([next(take) for _ in range(count)] for _ in range(4))
    w_out = [next(take) for _ in range(last)]
    new_half = [next(take) for _ in range(2)]
    new_pair = next(take)
    m_out, v_out, part, arrived = ([next(take) for _ in range(count)] for _ in range(4))
    shapes = max(kinds) + 1
    own, m_set, v_set, w_set = ([next(take) for _ in range(shapes)] for _ in range(4))
    own_sem, set_in, set_out, pair_send, pair_recv, ring_send, ring_recv, gather_send, gather_recv, local_sem = take

    me = lax.axis_index("dp")
    chip, core = me // CORES, me % CORES
    partner = chip * CORES + (1 - core)
    turn = [lax.rem(chip + d, chips) for d in range(chips)]
    right, left = turn[1] * CORES + core, turn[chips - 1] * CORES + core
    far = chips // 2

    chunks = [(a, layer) for a in range(count) for layer in range(layers)]
    rows = [r.shape[2] for r in part]
    half = [r // 2 for r in rows]

    def remote(src, dst, send, recv, to):
        return pltpu.make_async_remote_copy(src_ref=src, dst_ref=dst, send_sem=send, recv_sem=recv, device_id={"dp": to}, device_id_type=MESH)

    waits = []

    def finish_later(copy, *ends):
        copy.start()
        waits.extend(getattr(copy, end) for end in ends)

    order = ((far, 0), (far, 1), (1, 1), (chips - 1, 0), (1, 0), (chips - 1, 1), (0, 0), (0, 1))

    def pair_copy(j, d, h):
        a, layer = chunks[j]
        src = g[a].at[0, layer, pl.ds(pl.multiple_of((turn[d] * CORES + 1 - core) * rows[a] + h * half[a], STRIP), half[a])]
        s = j * len(order) + order.index((d, h))
        return remote(src, part[a].at[layer, d, pl.ds(h * half[a], half[a])], pair_send.at[s], pair_recv.at[s], partner)

    def start_pair(j):
        for d, h in order:
            finish_later(pair_copy(j, d, h), "wait_send")

    total = len(chunks)
    gathered = [j for j in range(total) if chunks[j][0] != last]
    plan = [("pair", 0)]
    for s in range(total):
        plan += [("first", s)]
        plan += [("pair", s + 1)] if s + 1 < total else []
        plan += [("middle", s - 1)] if s >= 1 else []
        plan += [("middle", s)] if s == total - 1 else []
        plan += [("final", s - 2)] if s >= 2 else []
        plan += [("pass", s - 4)] if s >= 4 else []
        plan += [("hand", s - 5)] if s >= 5 else []
    passed = [j for act, j in plan if act == "pass"]
    handed = [j for act, j in plan if act == "hand"]
    rest = [j for j in gathered if j not in passed]
    plan += [("pass", rest[0]), ("final", total - 2)]
    plan += [("pass", j) for j in rest[1:]] + [("final", total - 1)]
    plan += [("hand", j) for j in gathered if j not in handed]

    uses = []
    for act, j in plan:
        uses += [(j, d, h) for d, h in {"first": order[:4], "middle": order[4:6], "final": order[6:]}.get(act, ())]
    of_kind = [[u for u in uses if kinds[chunks[u[0]][0]] == q] for q in range(shapes)]

    def own_copy(q, i):
        j, d, h = of_kind[q][i]
        a, layer = chunks[j]
        src = g[a].at[0, layer, pl.ds(pl.multiple_of((turn[d] * CORES + core) * rows[a] + h * half[a], STRIP), half[a])]
        return pltpu.make_async_copy(src, own[q].at[i % SLOTS], own_sem.at[q, i % SLOTS])

    for q in range(shapes):
        for i in range(min(SLOTS, len(of_kind[q]))):
            own_copy(q, i).start()
    used = [0] * shapes

    def add_own(j, d, h, extra, finish=None):
        a, layer = chunks[j]
        q = kinds[a]
        i = used[q]
        used[q] += 1
        assert of_kind[q][i] == (j, d, h)
        pair_copy(j, d, h).wait_recv()
        own_copy(q, i).wait()
        mine = own[q].at[i % SLOTS]
        total = part[a].at[layer, d, pl.ds(h * half[a], half[a])]

        def body(strip):
            x = f32(total[strip, :]) + f32(mine[strip, :])
            for one in extra:
                x = x + f32(one[strip, :])
            x = x.astype(jnp.bfloat16)
            total[strip, :] = x if finish is None else finish(strip, f32(x))

        strips(half[a], body)
        if i + SLOTS < len(of_kind[q]):
            own_copy(q, i + SLOTS).start()
        return total

    def ring_copy(j, slot):
        a, layer = chunks[j]
        d, h = ((far, 0), (1, 1), (1, 0), (far, 1), (chips - 1, 0), (chips - 1, 1))[slot]
        src = part[a].at[layer, d, pl.ds(h * half[a], half[a])]
        s = j * 6 + slot
        return remote(src, arrived[a].at[layer, slot], ring_send.at[s], ring_recv.at[s], right if slot < 3 else left)

    def send(j, slot):
        finish_later(ring_copy(j, slot), "wait_send")

    def arrival(j, slot):
        ring_copy(j, slot).wait_recv()
        a, layer = chunks[j]
        return arrived[a].at[layer, slot]

    def first(j):
        add_own(j, far, 0, ())
        send(j, 0)
        add_own(j, far, 1, ())
        send(j, 3)
        add_own(j, 1, 1, ())
        send(j, 1)
        add_own(j, chips - 1, 0, ())
        send(j, 4)

    def middle(j):
        add_own(j, 1, 0, (arrival(j, 0),))
        send(j, 2)
        add_own(j, chips - 1, 1, (arrival(j, 3),))
        send(j, 5)

    units = [[(j, h) for j in range(len(chunks)) for h in range(2) if kinds[chunks[j][0]] == q] for q in range(shapes)]

    def set_copies(q, i):
        j, h = units[q][i]
        a, layer = chunks[j]
        cut = pl.ds(h * half[a], half[a])
        mine = pl.ds(pl.multiple_of(me * rows[a] + h * half[a], STRIP), half[a])
        t = i % SETS
        return [
            pltpu.make_async_copy(m[a].at[layer, cut], m_set[q].at[t], set_in.at[q, t, 0]),
            pltpu.make_async_copy(v[a].at[layer, cut], v_set[q].at[t], set_in.at[q, t, 1]),
            pltpu.make_async_copy(w[a].at[layer, mine], w_set[q].at[t], set_in.at[q, t, 2]),
        ], [
            pltpu.make_async_copy(m_set[q].at[t], m_out[a].at[layer, cut], set_out.at[q, t, 0]),
            pltpu.make_async_copy(v_set[q].at[t], v_out[a].at[layer, cut], set_out.at[q, t, 1]),
        ]

    def start_set(q, i):
        if i < len(units[q]):
            if i >= SETS:
                for copy in set_copies(q, i - SETS)[1]:
                    copy.wait()
            for copy in set_copies(q, i)[0]:
                copy.start()

    for q in range(shapes):
        for i in range(SETS - 1):
            start_set(q, i)

    def update(j, h, extra):
        a, _ = chunks[j]
        q = kinds[a]
        i = units[q].index((j, h))
        ins, outs = set_copies(q, i)
        for copy in ins:
            copy.wait()
        mm, vv, ww = (s[q].at[i % SETS] for s in (m_set, v_set, w_set))

        def finish(strip, grad):
            old = f32(ww[strip, :])
            new_m = 0.9 * mm[strip, :] + 0.1 * grad
            new_v = 0.95 * vv[strip, :] + 0.05 * grad * grad
            mm[strip, :] = new_m
            vv[strip, :] = new_v
            step = new_m * lax.rsqrt(new_v + 1e-8) + 0.1 * old
            return (old - 0.02 * step).astype(jnp.bfloat16)

        add_own(j, 0, h, extra, finish)
        for copy in outs:
            copy.start()
        start_set(q, i + SETS - 1)

    def block(a, layer, chip_of, core_of, h=None):
        base = (chip_of * CORES + core_of) * rows[a]
        if h is None:
            return w_out[a].at[layer, pl.ds(pl.multiple_of(base, STRIP), rows[a])]
        return w_out[a].at[layer, pl.ds(pl.multiple_of(base + h * half[a], STRIP), half[a])]

    def gather_copy(j, n):
        a, layer = chunks[j]
        s = (gather_send.at[j, n], gather_recv.at[j, n])
        mine = lambda h: part[a].at[layer, 0, pl.ds(h * half[a], half[a])]
        if n < 4:
            h, to = n % 2, right if n < 2 else left
            return remote(mine(h), block(a, layer, chip, core, h), *s, to)
        if n < 6:
            d, h, to = ((chips - 1, 0, right), (1, 1, left))[n - 4]
            there = block(a, layer, turn[d], core, h)
            return remote(there, there, *s, to)
        if n == 6:
            return remote(part[a].at[layer, 0], block(a, layer, chip, core), *s, partner)
        d, h = ((chips - 1, None), (1, None), (far, 0), (far, 1))[n - 7]
        there = block(a, layer, turn[d], core, h)
        return remote(there, there, *s, partner)

    def go(j, n):
        finish_later(gather_copy(j, n), "wait_send", *(("wait_recv",) if n >= 6 else ()))

    def final(j):
        a, layer = chunks[j]
        if a == last:
            for h, slots in enumerate(((2, 4), (1, 5))):
                update(j, h, [arrival(j, slot) for slot in slots])
                half_of = part[a].at[layer, 0, pl.ds(h * half[a], half[a])]
                finish_later(pltpu.make_async_copy(half_of, new_half[h].at[layer], local_sem.at[j, h]), "wait")
            pair = remote(part[a].at[layer, 0], new_pair.at[layer], gather_send.at[j, 6], gather_recv.at[j, 6], partner)
            finish_later(pair, "wait_send", "wait_recv")
            return
        update(j, 0, (arrival(j, 2), arrival(j, 4)))
        go(j, 0)
        update(j, 1, (arrival(j, 1), arrival(j, 5)))
        go(j, 3)
        go(j, 1)
        go(j, 2)
        go(j, 6)
        finish_later(pltpu.make_async_copy(part[a].at[layer, 0], block(a, layer, chip, core), local_sem.at[j, 0]), "wait")

    def pass_on(j):
        gather_copy(j, 0).wait_recv()
        go(j, 4)
        gather_copy(j, 3).wait_recv()
        go(j, 5)
        gather_copy(j, 1).wait_recv()
        go(j, 7)
        gather_copy(j, 2).wait_recv()
        go(j, 8)

    def hand_over(j):
        gather_copy(j, 4).wait_recv()
        go(j, 9)
        gather_copy(j, 5).wait_recv()
        go(j, 10)

    barrier = pltpu.get_barrier_semaphore()
    for other in (partner, right, left):
        pl.semaphore_signal(barrier, inc=1, device_id={"dp": other}, device_id_type=MESH)
    pl.semaphore_wait(barrier, 3)

    acts = {"pair": start_pair, "first": first, "middle": middle, "final": final, "pass": pass_on, "hand": hand_over}
    for act, j in plan:
        acts[act](j)

    for q in range(shapes):
        for i in range(max(0, len(units[q]) - SETS), len(units[q])):
            for copy in set_copies(q, i)[1]:
                copy.wait()
    for wait in waits:
        wait()


def moved(arrays, steps):
    def body(*refs):
        for src, dst in zip(refs[: len(arrays)], refs[len(arrays) :], strict=True):
            dst[...] = src[...]

    specs = [pl.BlockSpec((x.shape[0] // steps[0], x.shape[1] // steps[1], x.shape[2]), lambda i, j: (i, j, 0)) for x in arrays]
    size = sum(x.size * x.dtype.itemsize for x in arrays)
    return pl.pallas_call(
        body,
        out_shape=[jax.ShapeDtypeStruct(x.shape, x.dtype) for x in arrays],
        grid=steps,
        in_specs=specs,
        out_specs=specs,
        compiler_params=pltpu.CompilerParams(vmem_limit_bytes=VMEM),
        cost_estimate=pl.CostEstimate(flops=0, bytes_accessed=2 * size, transcendentals=0),
    )(*arrays)


def placed(shape, chips, into, pieces):
    arrays = [p[0] for p in pieces]
    count = len(arrays)

    def body(*refs):
        refs = refs[0 if into is None else 1 :]
        srcs, dst, bufs, sems = refs[:count], refs[count], refs[count + 1 : -1], refs[-1]
        me = lax.axis_index("dp")
        chip, core = me // CORES, me % CORES
        rows = shape[1] // (chips * CORES)
        ins, outs = [], []
        for n, (x, d, other, first) in enumerate(pieces):
            base = (lax.rem(chip + d, chips) * CORES + (1 - core if other else core)) * rows + first
            there = dst.at[:, pl.ds(pl.multiple_of(base, STRIP), x.shape[1])]
            ins.append(pltpu.make_async_copy(srcs[n], bufs[n], sems.at[n, 0]))
            outs.append(pltpu.make_async_copy(bufs[n], there, sems.at[n, 1]))
        for copy in ins:
            copy.start()
        for come, go in zip(ins, outs, strict=True):
            come.wait()
            go.start()
        for copy in outs:
            copy.wait()

    any_space = pl.BlockSpec(memory_space=pl.ANY)
    size = sum(x.size * x.dtype.itemsize for x in arrays)
    return pl.pallas_call(
        body,
        out_shape=jax.ShapeDtypeStruct(shape, arrays[0].dtype),
        in_specs=[any_space] * (count + (into is not None)),
        out_specs=any_space,
        scratch_shapes=[pltpu.VMEM(x.shape, x.dtype) for x in arrays] + [pltpu.SemaphoreType.DMA((count, 2))],
        input_output_aliases={} if into is None else {0: 0},
        compiler_params=pltpu.CompilerParams(vmem_limit_bytes=VMEM),
        cost_estimate=pl.CostEstimate(flops=0, bytes_accessed=2 * size, transcendentals=0),
    )(*(() if into is None else (into,)), *arrays)


def solution(mesh):
    devices = mesh.shape["dp"]
    chips = devices // CORES

    def hop(x, d):
        return lax.ppermute(x, "dp", [(i, (i + d * CORES) % devices) for i in range(devices)])

    def across(x):
        return lax.ppermute(x, "dp", [(i, i // CORES * CORES + 1 - i % CORES) for i in range(devices)])

    def step(*arrays):
        terms, weights, m, v = (arrays[i : i + 3] for i in (0, 3, 6, 9))
        count, layers = len(weights), weights[0].shape[0]
        blocks = [one.shape[1:] for one in m]
        distinct = list(dict.fromkeys(blocks))
        kinds = tuple(distinct.index(b) for b in blocks)
        chunks = count * layers
        any_space = pl.BlockSpec(memory_space=pl.ANY)
        bf16 = jnp.bfloat16
        halves = [(b[0] // 2, b[1]) for b in distinct]
        cut_rows = blocks[-1][0] // 2
        dma = pltpu.SemaphoreType.DMA
        tail = [jax.ShapeDtypeStruct((layers, cut_rows, blocks[-1][1]), bf16)] * 2 + [jax.ShapeDtypeStruct((layers, *blocks[-1]), bf16)]
        out = pl.pallas_call(
            functools.partial(kernel, chips, layers, kinds),
            out_shape=[jax.ShapeDtypeStruct(one.shape, one.dtype) for one in weights[:-1]]
            + tail
            + [jax.ShapeDtypeStruct(one.shape, one.dtype) for one in (*m, *v)],
            in_specs=[any_space] * 4 * count,
            out_specs=[any_space] * (3 * count + 2),
            scratch_shapes=[pltpu.VMEM((layers, chips, *b), bf16) for b in blocks]
            + [pltpu.VMEM((layers, 6, b[0] // 2, b[1]), bf16) for b in blocks]
            + [pltpu.VMEM((SLOTS, *b), bf16) for b in halves]
            + [pltpu.VMEM((SETS, *b), jnp.float32) for b in halves] * 2
            + [pltpu.VMEM((SETS, *b), bf16) for b in halves]
            + [dma((len(distinct), SLOTS)), dma((len(distinct), SETS, 3)), dma((len(distinct), SETS, 2))]
            + [dma((chunks * 2 * chips,))] * 2
            + [dma((chunks * 6,))] * 2
            + [dma((chunks, 11))] * 2
            + [dma((chunks, 2))],
            compiler_params=pltpu.CompilerParams(collective_id=0, has_side_effects=True, vmem_limit_bytes=VMEM),
        )(*terms, *weights, *m, *v)
        new, (own_a, own_b, pair), moments = out[: count - 1], out[count - 1 : count + 2], out[count + 2 :]
        shape, far, hold = weights[-1].shape, chips // 2, lax.optimization_barrier
        put = functools.partial(placed, shape, chips)
        left_a, right_b = hop(own_a, 1), hop(own_b, -1)
        left_b, right_a = hop(own_b, 1), hop(own_a, -1)
        results = moved([*new, *moments], (layers, chips))
        left_a, right_b, own_a, *results = hold((left_a, right_b, own_a, *results))
        far_a = hop(left_a, 1)
        far_b = hop(right_b, -1)
        over_left_a, over_right_b = across(left_a), across(right_b)
        whole = put(None, [(own_a, 0, 0, 0), (own_b, 0, 0, cut_rows), (pair, 0, 1, 0), (left_a, chips - 1, 0, 0), (right_b, 1, 0, cut_rows)])
        left_b, right_a, over_left_a, whole = hold((left_b, right_a, over_left_a, whole))
        over_left_b, over_right_a = across(left_b), across(right_a)
        whole = put(whole, [(left_b, chips - 1, 0, cut_rows), (right_a, 1, 0, 0), (over_left_a, chips - 1, 1, 0), (over_right_b, 1, 1, cut_rows)])
        over_left_b, over_right_a, whole = hold((over_left_b, over_right_a, whole))
        whole = put(whole, [(over_left_b, chips - 1, 1, cut_rows), (over_right_a, 1, 1, 0)])
        far_a, far_b, whole = hold((far_a, far_b, whole))
        over_far_a, over_far_b = across(far_a), across(far_b)
        whole = put(whole, [(far_a, far, 0, 0), (far_b, far, 0, cut_rows)])
        over_far_a, over_far_b, whole = hold((over_far_a, over_far_b, whole))
        whole = put(whole, [(over_far_a, far, 1, 0), (over_far_b, far, 1, cut_rows)])
        return (*results[: count - 1], whole, *results[count - 1 :])

    all_of, cut = P(None, None, None), P(None, "dp", None)
    return jax.shard_map(
        step,
        mesh=mesh,
        in_specs=(P(("rep", "dp"), None, None, None),) * 3 + (all_of,) * 3 + (cut,) * 6,
        out_specs=(P("rep", None, None),) * 3 + (P("rep", "dp", None),) * 6,
        check_vma=False,
    )
```

```python
import functools
import itertools

import jax
import jax.numpy as jnp
from jax import lax
from jax.experimental import pallas as pl
from jax.experimental.pallas import tpu as pltpu
from jax.sharding import PartitionSpec as P


MESH = pl.DeviceIdType.MESH
CORES = 2
STRIP = 16
SLOTS = 6
VMEM = 67043328
LEAD = 0
SETS = 3


def f32(x):
    return x.astype(jnp.float32)


def strips(rows, body):
    def one(i, carry):
        body(pl.ds(pl.multiple_of(i * STRIP, STRIP), STRIP))
        return carry

    lax.fori_loop(0, rows // STRIP, one, None)


def kernel(chips, layers, kinds, *refs):
    count = len(kinds)
    last = count - 1
    take = iter(refs)
    g, w, m, v = ([next(take) for _ in range(count)] for _ in range(4))
    w_out = [next(take) for _ in range(last)]
    new_half, new_pair, far_half = [next(take) for _ in range(2)], next(take), [next(take) for _ in range(2)]
    m_out, v_out, part, arrived = ([next(take) for _ in range(count)] for _ in range(4))
    shapes = max(kinds) + 1
    own, m_set, v_set, w_set = ([next(take) for _ in range(shapes)] for _ in range(4))
    own_sem, set_in, set_out, pair_send, pair_recv, ring_send, ring_recv, gather_send, gather_recv, local_sem, early_pair_send, early_pair_recv, early_ring_send, early_ring_recv, turn_sem = take

    me = lax.axis_index("dp")
    chip, core = me // CORES, me % CORES
    partner = chip * CORES + (1 - core)
    turn = [lax.rem(chip + d, chips) for d in range(chips)]
    right, left = turn[1] * CORES + core, turn[chips - 1] * CORES + core
    far = chips // 2

    chunks = [(a, layer) for a in range(count) for layer in range(layers)]
    rows = [r.shape[2] for r in part]
    half = [r // 2 for r in rows]

    def remote(src, dst, send, recv, to):
        return pltpu.make_async_remote_copy(src_ref=src, dst_ref=dst, send_sem=send, recv_sem=recv, device_id={"dp": to}, device_id_type=MESH)

    waits = []

    def finish_later(copy, *ends):
        copy.start()
        waits.extend(getattr(copy, end) for end in ends)

    order = ((far, 0), (far, 1), (1, 1), (chips - 1, 0), (1, 0), (chips - 1, 1), (0, 0), (0, 1))

    def pieces(j, d, h):
        size = half[chunks[j][0]]
        if j == 0 and d == far:
            return [(n, h * size + n * STRIP, STRIP) for n in range(size // STRIP)]
        return [(None, h * size, size)]

    def pair_copy(j, d, h, piece):
        a, layer = chunks[j]
        n, row, size = piece
        src = g[a].at[0, layer, pl.ds(pl.multiple_of((turn[d] * CORES + 1 - core) * rows[a] + row, STRIP), size)]
        s = j * len(order) + order.index((d, h))
        sems = (pair_send.at[s], pair_recv.at[s]) if n is None else (early_pair_send.at[h, n], early_pair_recv.at[h, n])
        return remote(src, part[a].at[layer, d, pl.ds(row, size)], *sems, partner)

    def start_pair(j):
        copies = [[(d, h, piece) for piece in pieces(j, d, h)] for d, h in order]
        for together in [*zip(*copies[:2], strict=True), *copies[2:]]:
            for one in together:
                finish_later(pair_copy(j, *one), "wait_send")

    total = len(chunks)
    gathered = [j for j in range(total) if chunks[j][0] != last]
    plan = [("pair", 0), ("follow", 0)]
    for s in range(total):
        plan += [("first", s)]
        plan += [("pair", s + 1)] if s + 1 < total else []
        plan += [("lead", s)] if s == 0 else []
        plan += [("middle", s - 1)] if s >= 1 else []
        plan += [("middle", s)] if s == total - 1 else []
        plan += [("final", s - 2)] if s >= 2 else []
        plan += [("pass", s - 4)] if s >= 4 else []
        plan += [("hand", s - 5)] if s >= 5 else []
    passed = [j for act, j in plan if act == "pass"]
    handed = [j for act, j in plan if act == "hand"]
    rest = [j for j in gathered if j not in passed]
    plan += [("pass", rest[0]), ("final", total - 2)]
    plan += [("pass", j) for j in rest[1:]] + [("final", total - 1)]
    plan += [("hand", j) for j in gathered if j not in handed]

    uses = []
    for act, j in plan:
        uses += [(j, d, h) for d, h in {"first": order[:4], "middle": order[4:6], "final": order[6:]}.get(act, ())]
    of_kind = [[u for u in uses if kinds[chunks[u[0]][0]] == q] for q in range(shapes)]

    def own_copy(q, i):
        j, d, h = of_kind[q][i]
        a, layer = chunks[j]
        src = g[a].at[0, layer, pl.ds(pl.multiple_of((turn[d] * CORES + core) * rows[a] + h * half[a], STRIP), half[a])]
        return pltpu.make_async_copy(src, own[q].at[i % SLOTS], own_sem.at[q, i % SLOTS])

    for q in range(shapes):
        for i in range(min(SLOTS, len(of_kind[q]))):
            own_copy(q, i).start()
    used = [0] * shapes

    def add_own(j, d, h, extra, finish=None):
        a, layer = chunks[j]
        q = kinds[a]
        i = used[q]
        used[q] += 1
        assert of_kind[q][i] == (j, d, h)
        own_copy(q, i).wait()
        mine = own[q].at[i % SLOTS]
        total = part[a].at[layer, d, pl.ds(h * half[a], half[a])]

        def body(strip):
            x = f32(total[strip, :]) + f32(mine[strip, :])
            for one in extra:
                x = x + f32(one[strip, :])
            x = x.astype(jnp.bfloat16)
            total[strip, :] = x if finish is None else finish(strip, f32(x))

        for piece in pieces(j, d, h):
            pair_copy(j, d, h, piece).wait_recv()
            if piece[0] is None:
                strips(half[a], body)
            else:
                body(pl.ds(piece[1] - h * half[a], piece[2]))
                yield piece
        if i + SLOTS < len(of_kind[q]):
            own_copy(q, i + SLOTS).start()

    def do(work):
        for _ in work:
            pass

    ring_slots = ((far, 0), (1, 1), (1, 0), (far, 1), (chips - 1, 0), (chips - 1, 1))

    def ring_copy(j, slot, piece):
        a, layer = chunks[j]
        n, row, size = piece
        d, h = ring_slots[slot]
        src = part[a].at[layer, d, pl.ds(row, size)]
        dst = arrived[a].at[layer, slot, pl.ds(row - h * half[a], size)]
        s = j * 6 + slot
        sems = (ring_send.at[s], ring_recv.at[s]) if n is None else (early_ring_send.at[h, n], early_ring_recv.at[h, n])
        return remote(src, dst, *sems, right if slot < 3 else left)

    def send(j, slot):
        for piece in pieces(j, *ring_slots[slot]):
            finish_later(ring_copy(j, slot, piece), "wait_send")

    come = set()

    def arrival(j, slot):
        for piece in [] if (j, slot) in come else pieces(j, *ring_slots[slot]):
            ring_copy(j, slot, piece).wait_recv()
        come.add((j, slot))
        a, layer = chunks[j]
        return arrived[a].at[layer, slot]

    def follow(j):
        @pl.when(core == 1)
        def _():
            pl.semaphore_wait(turn_sem, 1)

    def lead(j):
        arrival(j, LEAD)

        @pl.when(core == 0)
        def _():
            pl.semaphore_signal(turn_sem, inc=1, device_id={"dp": partner}, device_id_type=MESH)

    def add_and_send(j, slot, extra=()):
        do(add_own(j, *ring_slots[slot], extra))
        send(j, slot)

    def first(j):
        if pieces(j, far, 0)[0][0] is None:
            add_and_send(j, 0)
            add_and_send(j, 3)
        else:
            for both in itertools.zip_longest(add_own(j, far, 0, ()), add_own(j, far, 1, ())):
                for slot, piece in zip((0, 3), both, strict=True):
                    finish_later(ring_copy(j, slot, piece), "wait_send")
        add_and_send(j, 1)
        add_and_send(j, 4)

    def middle(j):
        add_and_send(j, 2, (arrival(j, 0),))
        add_and_send(j, 5, (arrival(j, 3),))

    units = [[(j, h) for j in range(len(chunks)) for h in range(2) if kinds[chunks[j][0]] == q] for q in range(shapes)]

    def set_copies(q, i):
        j, h = units[q][i]
        a, layer = chunks[j]
        cut = pl.ds(h * half[a], half[a])
        mine = pl.ds(pl.multiple_of(me * rows[a] + h * half[a], STRIP), half[a])
        t = i % SETS
        return [
            pltpu.make_async_copy(m[a].at[layer, cut], m_set[q].at[t], set_in.at[q, t, 0]),
            pltpu.make_async_copy(v[a].at[layer, cut], v_set[q].at[t], set_in.at[q, t, 1]),
            pltpu.make_async_copy(w[a].at[layer, mine], w_set[q].at[t], set_in.at[q, t, 2]),
        ], [
            pltpu.make_async_copy(m_set[q].at[t], m_out[a].at[layer, cut], set_out.at[q, t, 0]),
            pltpu.make_async_copy(v_set[q].at[t], v_out[a].at[layer, cut], set_out.at[q, t, 1]),
        ]

    def start_set(q, i):
        if i < len(units[q]):
            if i >= SETS:
                for copy in set_copies(q, i - SETS)[1]:
                    copy.wait()
            for copy in set_copies(q, i)[0]:
                copy.start()

    for q in range(shapes):
        for i in range(SETS - 1):
            start_set(q, i)

    def update(j, h, extra):
        a, _ = chunks[j]
        q = kinds[a]
        i = units[q].index((j, h))
        ins, outs = set_copies(q, i)
        for copy in ins:
            copy.wait()
        mm, vv, ww = (s[q].at[i % SETS] for s in (m_set, v_set, w_set))

        def finish(strip, grad):
            old = f32(ww[strip, :])
            new_m = 0.9 * mm[strip, :] + 0.1 * grad
            new_v = 0.95 * vv[strip, :] + 0.05 * grad * grad
            mm[strip, :] = new_m
            vv[strip, :] = new_v
            step = new_m * lax.rsqrt(new_v + 1e-8) + 0.1 * old
            return (old - 0.02 * step).astype(jnp.bfloat16)

        do(add_own(j, 0, h, extra, finish))
        for copy in outs:
            copy.start()
        start_set(q, i + SETS - 1)

    def block(a, layer, chip_of, core_of, h=None):
        base = (chip_of * CORES + core_of) * rows[a]
        if h is None:
            return w_out[a].at[layer, pl.ds(pl.multiple_of(base, STRIP), rows[a])]
        return w_out[a].at[layer, pl.ds(pl.multiple_of(base + h * half[a], STRIP), half[a])]

    def gather_copy(j, n):
        a, layer = chunks[j]
        s = (gather_send.at[j, n], gather_recv.at[j, n])
        mine = lambda h: part[a].at[layer, 0, pl.ds(h * half[a], half[a])]
        if n < 4:
            h, to = n % 2, right if n < 2 else left
            return remote(mine(h), block(a, layer, chip, core, h), *s, to)
        if n < 6:
            d, h, to = ((chips - 1, 0, right), (1, 1, left))[n - 4]
            there = block(a, layer, turn[d], core, h)
            return remote(there, far_half[h].at[layer] if a == last - 1 else there, *s, to)
        if n == 6:
            return remote(part[a].at[layer, 0], block(a, layer, chip, core), *s, partner)
        d, h = ((chips - 1, None), (1, None), (far, 0), (far, 1))[n - 7]
        there = block(a, layer, turn[d], core, h)
        return remote(there, there, *s, partner)

    def go(j, n):
        finish_later(gather_copy(j, n), "wait_send", *(("wait_recv",) if n >= 6 else ()))

    def final(j):
        a, layer = chunks[j]
        if a == last:
            for h, slots in enumerate(((2, 4), (1, 5))):
                update(j, h, [arrival(j, slot) for slot in slots])
                half_of = part[a].at[layer, 0, pl.ds(h * half[a], half[a])]
                finish_later(pltpu.make_async_copy(half_of, new_half[h].at[layer], local_sem.at[j, h]), "wait")
            pair = remote(part[a].at[layer, 0], new_pair.at[layer], gather_send.at[j, 6], gather_recv.at[j, 6], partner)
            finish_later(pair, "wait_send", "wait_recv")
            return
        update(j, 0, (arrival(j, 2), arrival(j, 4)))
        go(j, 0)
        update(j, 1, (arrival(j, 1), arrival(j, 5)))
        go(j, 3)
        go(j, 1)
        go(j, 2)
        go(j, 6)
        finish_later(pltpu.make_async_copy(part[a].at[layer, 0], block(a, layer, chip, core), local_sem.at[j, 0]), "wait")

    def pass_on(j):
        gather_copy(j, 0).wait_recv()
        go(j, 4)
        gather_copy(j, 3).wait_recv()
        go(j, 5)
        gather_copy(j, 1).wait_recv()
        go(j, 7)
        gather_copy(j, 2).wait_recv()
        go(j, 8)

    def hand_over(j):
        for n, then in ((4, 9), (5, 10)):
            gather_copy(j, n).wait_recv()
            if chunks[j][0] != last - 1:
                go(j, then)

    barrier = pltpu.get_barrier_semaphore()
    for other in (partner, right, left):
        pl.semaphore_signal(barrier, inc=1, device_id={"dp": other}, device_id_type=MESH)
    pl.semaphore_wait(barrier, 3)

    acts = {"pair": start_pair, "follow": follow, "lead": lead, "first": first, "middle": middle, "final": final, "pass": pass_on, "hand": hand_over}
    for act, j in plan:
        acts[act](j)

    for q in range(shapes):
        for i in range(max(0, len(units[q]) - SETS), len(units[q])):
            for copy in set_copies(q, i)[1]:
                copy.wait()
    for wait in waits:
        wait()


def moved(arrays, steps):
    def body(*refs):
        for src, dst in zip(refs[: len(arrays)], refs[len(arrays) :], strict=True):
            dst[...] = src[...]

    specs = [pl.BlockSpec((x.shape[0] // steps[0], x.shape[1] // steps[1], x.shape[2]), lambda i, j: (i, j, 0)) for x in arrays]
    size = sum(x.size * x.dtype.itemsize for x in arrays)
    return pl.pallas_call(
        body,
        out_shape=[jax.ShapeDtypeStruct(x.shape, x.dtype) for x in arrays],
        grid=steps,
        in_specs=specs,
        out_specs=specs,
        compiler_params=pltpu.CompilerParams(vmem_limit_bytes=VMEM),
        cost_estimate=pl.CostEstimate(flops=0, bytes_accessed=2 * size, transcendentals=0),
    )(*arrays)


def placed(shape, chips, into, pieces):
    arrays = [p[0] for p in pieces]
    count = len(arrays)

    def body(*refs):
        refs = refs[0 if into is None else 1 :]
        srcs, dst, bufs, sems = refs[:count], refs[count], refs[count + 1 : -1], refs[-1]
        me = lax.axis_index("dp")
        chip, core = me // CORES, me % CORES
        rows = shape[1] // (chips * CORES)
        ins, outs = [], []
        for n, (x, d, other, first) in enumerate(pieces):
            base = (lax.rem(chip + d, chips) * CORES + (1 - core if other else core)) * rows + first
            there = dst.at[:, pl.ds(pl.multiple_of(base, STRIP), x.shape[1])]
            ins.append(pltpu.make_async_copy(srcs[n], bufs[n], sems.at[n, 0]))
            outs.append(pltpu.make_async_copy(bufs[n], there, sems.at[n, 1]))
        for copy in ins:
            copy.start()
        for come, go in zip(ins, outs, strict=True):
            come.wait()
            go.start()
        for copy in outs:
            copy.wait()

    any_space = pl.BlockSpec(memory_space=pl.ANY)
    size = sum(x.size * x.dtype.itemsize for x in arrays)
    return pl.pallas_call(
        body,
        out_shape=jax.ShapeDtypeStruct(shape, arrays[0].dtype),
        in_specs=[any_space] * (count + (into is not None)),
        out_specs=any_space,
        scratch_shapes=[pltpu.VMEM(x.shape, x.dtype) for x in arrays] + [pltpu.SemaphoreType.DMA((count, 2))],
        input_output_aliases={} if into is None else {0: 0},
        compiler_params=pltpu.CompilerParams(vmem_limit_bytes=VMEM),
        cost_estimate=pl.CostEstimate(flops=0, bytes_accessed=2 * size, transcendentals=0),
    )(*(() if into is None else (into,)), *arrays)


def solution(mesh):
    devices = mesh.shape["dp"]
    chips = devices // CORES

    def hop(x, d):
        return lax.ppermute(x, "dp", [(i, (i + d * CORES) % devices) for i in range(devices)])

    def across(x):
        return lax.ppermute(x, "dp", [(i, i // CORES * CORES + 1 - i % CORES) for i in range(devices)])

    def step(*arrays):
        terms, weights, m, v = (arrays[i : i + 3] for i in (0, 3, 6, 9))
        count, layers = len(weights), weights[0].shape[0]
        blocks = [one.shape[1:] for one in m]
        distinct = list(dict.fromkeys(blocks))
        kinds = tuple(distinct.index(b) for b in blocks)
        chunks = count * layers
        any_space = pl.BlockSpec(memory_space=pl.ANY)
        bf16 = jnp.bfloat16
        halves = [(b[0] // 2, b[1]) for b in distinct]
        cut_rows = blocks[-1][0] // 2
        dma = pltpu.SemaphoreType.DMA
        cut_cols, (far_rows, far_cols) = blocks[-1][1], (blocks[-2][0] // 2, blocks[-2][1])
        tail = [(layers, cut_rows, cut_cols)] * 2 + [(layers, *blocks[-1])] + [(layers, far_rows, far_cols)] * 2
        early = (2, blocks[0][0] // 2 // STRIP)
        out = pl.pallas_call(
            functools.partial(kernel, chips, layers, kinds),
            out_shape=[jax.ShapeDtypeStruct(one.shape, one.dtype) for one in weights[:-1]]
            + [jax.ShapeDtypeStruct(one, bf16) for one in tail]
            + [jax.ShapeDtypeStruct(one.shape, one.dtype) for one in (*m, *v)],
            in_specs=[any_space] * 4 * count,
            out_specs=[any_space] * (3 * count - 1 + len(tail)),
            scratch_shapes=[pltpu.VMEM((layers, chips, *b), bf16) for b in blocks]
            + [pltpu.VMEM((layers, 6, b[0] // 2, b[1]), bf16) for b in blocks]
            + [pltpu.VMEM((SLOTS, *b), bf16) for b in halves]
            + [pltpu.VMEM((SETS, *b), jnp.float32) for b in halves] * 2
            + [pltpu.VMEM((SETS, *b), bf16) for b in halves]
            + [dma((len(distinct), SLOTS)), dma((len(distinct), SETS, 3)), dma((len(distinct), SETS, 2))]
            + [dma((chunks * 2 * chips,))] * 2
            + [dma((chunks * 6,))] * 2
            + [dma((chunks, 11))] * 2
            + [dma((chunks, 2))]
            + [dma(early)] * 4
            + [pltpu.SemaphoreType.REGULAR],
            compiler_params=pltpu.CompilerParams(collective_id=0, has_side_effects=True, vmem_limit_bytes=VMEM),
        )(*terms, *weights, *m, *v)
        new, (own_a, own_b, pair, late_a, late_b), moments = out[: count - 1], out[count - 1 : count - 1 + len(tail)], out[count - 1 + len(tail) :]
        shape, far, hold = weights[-1].shape, chips // 2, lax.optimization_barrier
        put = functools.partial(placed, shape, chips)
        left_a, right_b = hop(own_a, 1), hop(own_b, -1)
        left_b, right_a = hop(own_b, 1), hop(own_a, -1)
        results = list(moved([*new, *moments], (layers, chips)))
        left_a, right_b, own_a, results = hold((left_a, right_b, own_a, results))
        far_a, far_b = hop(left_a, 1), hop(right_b, -1)
        start = [(own_a, 0, 0, 0), (own_b, 0, 0, cut_rows), (pair, 0, 1, 0), (left_a, chips - 1, 0, 0), (right_b, 1, 0, cut_rows)]
        whole = put(None, start)
        left_a, right_b, left_b, right_a, late_a, late_b, whole = hold((left_a, right_b, left_b, right_a, late_a, late_b, whole))
        over = [across(x) for x in (left_a, right_b, left_b, right_a)]
        over_late = across(late_a), across(late_b)
        whole = put(whole, [(left_b, chips - 1, 0, cut_rows), (right_a, 1, 0, 0)])
        over, whole = hold((over, whole))
        whole = put(whole, [(x, d, 1, row) for x, d, row in zip(over, (chips - 1, 1, chips - 1, 1), (0, cut_rows, cut_rows, 0), strict=True)])
        over_late, whole, results = hold((over_late, whole, results))
        late = [(x, far, other, row) for other, two in enumerate(((late_a, late_b), over_late)) for x, row in zip(two, (0, far_rows), strict=True)]
        results[count - 2] = placed(weights[-2].shape, chips, results[count - 2], late)
        far_a, far_b, whole, results = hold((far_a, far_b, whole, results))
        over_far_a, over_far_b = across(far_a), across(far_b)
        whole = put(whole, [(far_a, far, 0, 0), (far_b, far, 0, cut_rows)])
        over_far_a, over_far_b, whole = hold((over_far_a, over_far_b, whole))
        whole = put(whole, [(over_far_a, far, 1, 0), (over_far_b, far, 1, cut_rows)])
        return (*results[: count - 1], whole, *results[count - 1 :])

    all_of, cut = P(None, None, None), P(None, "dp", None)
    return jax.shard_map(
        step,
        mesh=mesh,
        in_specs=(P(("rep", "dp"), None, None, None),) * 3 + (all_of,) * 3 + (cut,) * 6,
        out_specs=(P("rep", None, None),) * 3 + (P("rep", "dp", None),) * 6,
        check_vma=False,
    )
```

```python
import functools
import itertools

import jax
import jax.numpy as jnp
from jax import lax
from jax.experimental import pallas as pl
from jax.experimental.pallas import tpu as pltpu
from jax.sharding import PartitionSpec as P


MESH = pl.DeviceIdType.MESH
CORES = 2
STRIP = 16
SLOTS = 6
VMEM = 67043328
LEAD = 0
SETS = 3


def f32(x):
    return x.astype(jnp.float32)


def strips(rows, body):
    def one(i, carry):
        body(pl.ds(pl.multiple_of(i * STRIP, STRIP), STRIP))
        return carry

    lax.fori_loop(0, rows // STRIP, one, None)


def kernel(chips, layers, kinds, *refs):
    count = len(kinds)
    last = count - 1
    take = iter(refs)
    g, w, m, v = ([next(take) for _ in range(count)] for _ in range(4))
    w_out = [next(take) for _ in range(last)]
    new_half, new_pair, far_half = [next(take) for _ in range(2)], next(take), [next(take) for _ in range(2)]
    m_out, v_out, part, arrived = ([next(take) for _ in range(count)] for _ in range(4))
    shapes = max(kinds) + 1
    own, m_set, v_set, w_set = ([next(take) for _ in range(shapes)] for _ in range(4))
    own_sem, set_in, set_out, pair_send, pair_recv, ring_send, ring_recv, gather_send, gather_recv, local_sem, early_pair_send, early_pair_recv, early_ring_send, early_ring_recv, turn_sem = take

    me = lax.axis_index("dp")
    chip, core = me // CORES, me % CORES
    partner = chip * CORES + (1 - core)
    turn = [lax.rem(chip + d, chips) for d in range(chips)]
    right, left = turn[1] * CORES + core, turn[chips - 1] * CORES + core
    far = chips // 2

    chunks = [(a, layer) for a in range(count) for layer in range(layers)]
    rows = [r.shape[2] for r in part]
    half = [r // 2 for r in rows]

    def remote(src, dst, send, recv, to):
        return pltpu.make_async_remote_copy(src_ref=src, dst_ref=dst, send_sem=send, recv_sem=recv, device_id={"dp": to}, device_id_type=MESH)

    waits = []

    def finish_later(copy, *ends):
        copy.start()
        waits.extend(getattr(copy, end) for end in ends)

    order = ((far, 0), (far, 1), (1, 1), (chips - 1, 0), (1, 0), (chips - 1, 1), (0, 0), (0, 1))

    def pieces(j, d, h):
        size = half[chunks[j][0]]
        if j == 0 and d == far:
            return [(n, h * size + n * STRIP, STRIP) for n in range(size // STRIP)]
        return [(None, h * size, size)]

    def pair_copy(j, d, h, piece):
        a, layer = chunks[j]
        n, row, size = piece
        src = g[a].at[0, layer, pl.ds(pl.multiple_of((turn[d] * CORES + 1 - core) * rows[a] + row, STRIP), size)]
        s = j * len(order) + order.index((d, h))
        sems = (pair_send.at[s], pair_recv.at[s]) if n is None else (early_pair_send.at[h, n], early_pair_recv.at[h, n])
        return remote(src, part[a].at[layer, d, pl.ds(row, size)], *sems, partner)

    def start_pair(j):
        copies = [[(d, h, piece) for piece in pieces(j, d, h)] for d, h in order]
        for together in [*zip(*copies[:2], strict=True), *copies[2:]]:
            for one in together:
                finish_later(pair_copy(j, *one), "wait_send")

    total = len(chunks)
    gathered = [j for j in range(total) if chunks[j][0] != last]
    plan = [("pair", 0), ("follow", 0)]
    for s in range(total):
        plan += [("first", s)]
        plan += [("pair", s + 1)] if s + 1 < total else []
        plan += [("lead", s)] if s == 0 else []
        plan += [("middle", s - 1)] if s >= 1 else []
        plan += [("middle", s)] if s == total - 1 else []
        plan += [("final", s - 2)] if s >= 2 else []
        plan += [("pass", s - 4)] if s >= 4 else []
        plan += [("hand", s - 5)] if s >= 5 else []
    passed = [j for act, j in plan if act == "pass"]
    handed = [j for act, j in plan if act == "hand"]
    rest = [j for j in gathered if j not in passed]
    plan += [("pass", rest[0]), ("final", total - 2)]
    plan += [("pass", j) for j in rest[1:]] + [("final", total - 1)]
    plan += [("hand", j) for j in gathered if j not in handed]

    uses = []
    for act, j in plan:
        uses += [(j, d, h) for d, h in {"first": order[:4], "middle": order[4:6], "final": order[6:]}.get(act, ())]
    of_kind = [[u for u in uses if kinds[chunks[u[0]][0]] == q] for q in range(shapes)]

    def own_copy(q, i):
        j, d, h = of_kind[q][i]
        a, layer = chunks[j]
        src = g[a].at[0, layer, pl.ds(pl.multiple_of((turn[d] * CORES + core) * rows[a] + h * half[a], STRIP), half[a])]
        return pltpu.make_async_copy(src, own[q].at[i % SLOTS], own_sem.at[q, i % SLOTS])

    for q in range(shapes):
        for i in range(min(SLOTS, len(of_kind[q]))):
            own_copy(q, i).start()
    used = [0] * shapes

    def add_own(j, d, h, extra, finish=None):
        a, layer = chunks[j]
        q = kinds[a]
        i = used[q]
        used[q] += 1
        assert of_kind[q][i] == (j, d, h)
        own_copy(q, i).wait()
        mine = own[q].at[i % SLOTS]
        total = part[a].at[layer, d, pl.ds(h * half[a], half[a])]

        def body(strip):
            x = f32(total[strip, :]) + f32(mine[strip, :])
            for one in extra:
                x = x + f32(one[strip, :])
            x = x.astype(jnp.bfloat16)
            total[strip, :] = x if finish is None else finish(strip, f32(x))

        for piece in pieces(j, d, h):
            pair_copy(j, d, h, piece).wait_recv()
            if piece[0] is None:
                strips(half[a], body)
            else:
                body(pl.ds(piece[1] - h * half[a], piece[2]))
                yield piece
        if i + SLOTS < len(of_kind[q]):
            own_copy(q, i + SLOTS).start()

    def do(work):
        for _ in work:
            pass

    ring_slots = ((far, 0), (1, 1), (1, 0), (far, 1), (chips - 1, 0), (chips - 1, 1))

    def ring_copy(j, slot, piece):
        a, layer = chunks[j]
        n, row, size = piece
        d, h = ring_slots[slot]
        src = part[a].at[layer, d, pl.ds(row, size)]
        dst = arrived[a].at[layer, slot, pl.ds(row - h * half[a], size)]
        s = j * 6 + slot
        sems = (ring_send.at[s], ring_recv.at[s]) if n is None else (early_ring_send.at[h, n], early_ring_recv.at[h, n])
        return remote(src, dst, *sems, right if slot < 3 else left)

    def send(j, slot):
        for piece in pieces(j, *ring_slots[slot]):
            finish_later(ring_copy(j, slot, piece), "wait_send")

    come = set()

    def arrival(j, slot):
        for piece in [] if (j, slot) in come else pieces(j, *ring_slots[slot]):
            ring_copy(j, slot, piece).wait_recv()
        come.add((j, slot))
        a, layer = chunks[j]
        return arrived[a].at[layer, slot]

    def follow(j):
        @pl.when(core == 1)
        def _():
            pl.semaphore_wait(turn_sem, 1)

    def lead(j):
        arrival(j, LEAD)

        @pl.when(core == 0)
        def _():
            pl.semaphore_signal(turn_sem, inc=1, device_id={"dp": partner}, device_id_type=MESH)

    def add_and_send(j, slot, extra=()):
        do(add_own(j, *ring_slots[slot], extra))
        send(j, slot)

    def first(j):
        if pieces(j, far, 0)[0][0] is None:
            add_and_send(j, 0)
            add_and_send(j, 3)
        else:
            for both in itertools.zip_longest(add_own(j, far, 0, ()), add_own(j, far, 1, ())):
                for slot, piece in zip((0, 3), both, strict=True):
                    finish_later(ring_copy(j, slot, piece), "wait_send")
        add_and_send(j, 1)
        add_and_send(j, 4)

    def middle(j):
        add_and_send(j, 2, (arrival(j, 0),))
        add_and_send(j, 5, (arrival(j, 3),))

    units = [[(j, h) for j in range(len(chunks)) for h in range(2) if kinds[chunks[j][0]] == q] for q in range(shapes)]

    def set_copies(q, i):
        j, h = units[q][i]
        a, layer = chunks[j]
        cut = pl.ds(h * half[a], half[a])
        mine = pl.ds(pl.multiple_of(me * rows[a] + h * half[a], STRIP), half[a])
        t = i % SETS
        return [
            pltpu.make_async_copy(m[a].at[layer, cut], m_set[q].at[t], set_in.at[q, t, 0]),
            pltpu.make_async_copy(v[a].at[layer, cut], v_set[q].at[t], set_in.at[q, t, 1]),
            pltpu.make_async_copy(w[a].at[layer, mine], w_set[q].at[t], set_in.at[q, t, 2]),
        ], [
            pltpu.make_async_copy(m_set[q].at[t], m_out[a].at[layer, cut], set_out.at[q, t, 0]),
            pltpu.make_async_copy(v_set[q].at[t], v_out[a].at[layer, cut], set_out.at[q, t, 1]),
        ]

    def start_set(q, i):
        if i < len(units[q]):
            if i >= SETS:
                for copy in set_copies(q, i - SETS)[1]:
                    copy.wait()
            for copy in set_copies(q, i)[0]:
                copy.start()

    for q in range(shapes):
        for i in range(SETS - 1):
            start_set(q, i)

    def update(j, h, extra):
        a, _ = chunks[j]
        q = kinds[a]
        i = units[q].index((j, h))
        ins, outs = set_copies(q, i)
        for copy in ins:
            copy.wait()
        mm, vv, ww = (s[q].at[i % SETS] for s in (m_set, v_set, w_set))

        def finish(strip, grad):
            old = f32(ww[strip, :])
            new_m = 0.9 * mm[strip, :] + 0.1 * grad
            new_v = 0.95 * vv[strip, :] + 0.05 * grad * grad
            mm[strip, :] = new_m
            vv[strip, :] = new_v
            step = new_m * lax.rsqrt(new_v + 1e-8) + 0.1 * old
            return (old - 0.02 * step).astype(jnp.bfloat16)

        do(add_own(j, 0, h, extra, finish))
        for copy in outs:
            copy.start()
        start_set(q, i + SETS - 1)

    def block(a, layer, chip_of, core_of, h=None):
        base = (chip_of * CORES + core_of) * rows[a]
        if h is None:
            return w_out[a].at[layer, pl.ds(pl.multiple_of(base, STRIP), rows[a])]
        return w_out[a].at[layer, pl.ds(pl.multiple_of(base + h * half[a], STRIP), half[a])]

    def gather_copy(j, n):
        a, layer = chunks[j]
        s = (gather_send.at[j, n], gather_recv.at[j, n])
        mine = lambda h: part[a].at[layer, 0, pl.ds(h * half[a], half[a])]
        if n < 4:
            h, to = n % 2, right if n < 2 else left
            return remote(mine(h), block(a, layer, chip, core, h), *s, to)
        if n < 6:
            d, h, to = ((chips - 1, 0, right), (1, 1, left))[n - 4]
            there = block(a, layer, turn[d], core, h)
            return remote(there, far_half[h].at[layer] if a == last - 1 else there, *s, to)
        if n == 6:
            return remote(part[a].at[layer, 0], block(a, layer, chip, core), *s, partner)
        d, h = ((chips - 1, None), (1, None), (far, 0), (far, 1))[n - 7]
        there = block(a, layer, turn[d], core, h)
        return remote(there, there, *s, partner)

    def go(j, n):
        finish_later(gather_copy(j, n), "wait_send", *(("wait_recv",) if n >= 6 else ()))

    def final(j):
        a, layer = chunks[j]
        if a == last:
            for h, slots in enumerate(((2, 4), (1, 5))):
                update(j, h, [arrival(j, slot) for slot in slots])
                half_of = part[a].at[layer, 0, pl.ds(h * half[a], half[a])]
                finish_later(pltpu.make_async_copy(half_of, new_half[h].at[layer], local_sem.at[j, h]), "wait")
            pair = remote(part[a].at[layer, 0], new_pair.at[layer], gather_send.at[j, 6], gather_recv.at[j, 6], partner)
            finish_later(pair, "wait_send", "wait_recv")
            return
        update(j, 0, (arrival(j, 2), arrival(j, 4)))
        go(j, 0)
        update(j, 1, (arrival(j, 1), arrival(j, 5)))
        go(j, 3)
        go(j, 1)
        go(j, 2)
        go(j, 6)
        finish_later(pltpu.make_async_copy(part[a].at[layer, 0], block(a, layer, chip, core), local_sem.at[j, 0]), "wait")

    def pass_on(j):
        gather_copy(j, 0).wait_recv()
        go(j, 4)
        gather_copy(j, 3).wait_recv()
        go(j, 5)
        gather_copy(j, 1).wait_recv()
        go(j, 7)
        gather_copy(j, 2).wait_recv()
        go(j, 8)

    def hand_over(j):
        for n, then in ((4, 9), (5, 10)):
            gather_copy(j, n).wait_recv()
            if chunks[j][0] != last - 1:
                go(j, then)

    barrier = pltpu.get_barrier_semaphore()
    for other in (partner, right, left):
        pl.semaphore_signal(barrier, inc=1, device_id={"dp": other}, device_id_type=MESH)
    pl.semaphore_wait(barrier, 3)

    acts = {"pair": start_pair, "follow": follow, "lead": lead, "first": first, "middle": middle, "final": final, "pass": pass_on, "hand": hand_over}
    for act, j in plan:
        acts[act](j)

    for q in range(shapes):
        for i in range(max(0, len(units[q]) - SETS), len(units[q])):
            for copy in set_copies(q, i)[1]:
                copy.wait()
    for wait in waits:
        wait()


def relayed(targets, pieces):
    arrays = list({id(p[1]): p[1] for p in pieces}.values())
    at = {id(x): n for n, x in enumerate(arrays)}
    intos = [(n, t) for n, t in enumerate(targets) if not isinstance(t, jax.ShapeDtypeStruct)]

    def body(*refs):
        take = iter(refs[len(intos) :])
        srcs, dsts, bufs = ([next(take) for _ in one] for one in (arrays, targets, pieces))
        sems = next(take)
        me = lax.axis_index("dp")
        place = me // CORES, me % CORES
        ins, outs = [], []
        for n, (t, x, _, here, there) in enumerate(pieces):
            ins.append(pltpu.make_async_copy(srcs[at[id(x)]].at[here(*place)], bufs[n], sems.at[n, 0]))
            outs.append(pltpu.make_async_copy(bufs[n], dsts[t].at[there(*place)], sems.at[n, 1]))
        for copy in ins:
            copy.start()
        for come, go in zip(ins, outs, strict=True):
            come.wait()
            go.start()
        for copy in outs:
            copy.wait()

    any_space = pl.BlockSpec(memory_space=pl.ANY)
    return pl.pallas_call(
        body,
        out_shape=[jax.ShapeDtypeStruct(t.shape, t.dtype) for t in targets],
        in_specs=[any_space] * (len(intos) + len(arrays)),
        out_specs=[any_space] * len(targets),
        scratch_shapes=[pltpu.VMEM(shape, x.dtype) for _, x, shape, *_ in pieces] + [pltpu.SemaphoreType.DMA((len(pieces), 2))],
        input_output_aliases={i: n for i, (n, _) in enumerate(intos)},
        compiler_params=pltpu.CompilerParams(vmem_limit_bytes=VMEM),
    )(*[t for _, t in intos], *arrays)


def moved(arrays, steps, hole):
    def body(*refs):
        for src, dst in zip(refs[: len(arrays)], refs[len(arrays) :], strict=True):
            dst[...] = src[...]

    def spec(n, x):
        def at(i, j):
            if n != hole[0]:
                return i, j, 0
            step = jnp.where(j == hole[1], j - 1, j)
            return i, lax.rem(lax.axis_index("dp") // CORES + step, steps[1]), 0

        return pl.BlockSpec((x.shape[0] // steps[0], x.shape[1] // steps[1], x.shape[2]), at)

    specs = [spec(n, x) for n, x in enumerate(arrays)]
    return pl.pallas_call(
        body,
        out_shape=[jax.ShapeDtypeStruct(x.shape, x.dtype) for x in arrays],
        grid=steps,
        in_specs=specs,
        out_specs=specs,
        compiler_params=pltpu.CompilerParams(vmem_limit_bytes=VMEM),
    )(*arrays)


def placed(chips, targets, blocks):
    def piece(t, x, d, other, first):
        rows = targets[t].shape[1] // (chips * CORES)

        def there(chip, core):
            base = (lax.rem(chip + d, chips) * CORES + (1 - core if other else core)) * rows + first
            return (slice(None), pl.ds(pl.multiple_of(base, STRIP), x.shape[1]))

        return (t, x, x.shape, lambda chip, core: slice(None), there)

    return relayed(targets, [piece(*one) for one in blocks])


def solution(mesh):
    devices = mesh.shape["dp"]
    chips = devices // CORES

    def hop(x, d):
        return lax.ppermute(x, "dp", [(i, (i + d * CORES) % devices) for i in range(devices)])

    def across(x):
        return lax.ppermute(x, "dp", [(i, i // CORES * CORES + 1 - i % CORES) for i in range(devices)])

    def step(*arrays):
        terms, weights, m, v = (arrays[i : i + 3] for i in (0, 3, 6, 9))
        count, layers = len(weights), weights[0].shape[0]
        blocks = [one.shape[1:] for one in m]
        distinct = list(dict.fromkeys(blocks))
        kinds = tuple(distinct.index(b) for b in blocks)
        chunks = count * layers
        any_space = pl.BlockSpec(memory_space=pl.ANY)
        bf16 = jnp.bfloat16
        halves = [(b[0] // 2, b[1]) for b in distinct]
        cut_rows = blocks[-1][0] // 2
        dma = pltpu.SemaphoreType.DMA
        cut_cols, (far_rows, far_cols) = blocks[-1][1], (blocks[-2][0] // 2, blocks[-2][1])
        tail = [(layers, cut_rows, cut_cols)] * 2 + [(layers, *blocks[-1])] + [(layers, far_rows, far_cols)] * 2
        early = (2, blocks[0][0] // 2 // STRIP)
        out = pl.pallas_call(
            functools.partial(kernel, chips, layers, kinds),
            out_shape=[jax.ShapeDtypeStruct(one.shape, one.dtype) for one in weights[:-1]]
            + [jax.ShapeDtypeStruct(one, bf16) for one in tail]
            + [jax.ShapeDtypeStruct(one.shape, one.dtype) for one in (*m, *v)],
            in_specs=[any_space] * 4 * count,
            out_specs=[any_space] * (3 * count - 1 + len(tail)),
            scratch_shapes=[pltpu.VMEM((layers, chips, *b), bf16) for b in blocks]
            + [pltpu.VMEM((layers, 6, b[0] // 2, b[1]), bf16) for b in blocks]
            + [pltpu.VMEM((SLOTS, *b), bf16) for b in halves]
            + [pltpu.VMEM((SETS, *b), jnp.float32) for b in halves] * 2
            + [pltpu.VMEM((SETS, *b), bf16) for b in halves]
            + [dma((len(distinct), SLOTS)), dma((len(distinct), SETS, 3)), dma((len(distinct), SETS, 2))]
            + [dma((chunks * 2 * chips,))] * 2
            + [dma((chunks * 6,))] * 2
            + [dma((chunks, 11))] * 2
            + [dma((chunks, 2))]
            + [dma(early)] * 4
            + [pltpu.SemaphoreType.REGULAR],
            compiler_params=pltpu.CompilerParams(collective_id=0, has_side_effects=True, vmem_limit_bytes=VMEM),
        )(*terms, *weights, *m, *v)
        new, (own_a, own_b, pair, late_a, late_b), moments = out[: count - 1], out[count - 1 : count - 1 + len(tail)], out[count - 1 + len(tail) :]
        far, hold = chips // 2, lax.optimization_barrier
        back, down = chips - 1, cut_rows
        put = functools.partial(placed, chips)
        left_a, right_b = hop(own_a, 1), hop(own_b, -1)
        left_b, right_a = hop(own_b, 1), hop(own_a, -1)
        results = list(moved([*new, *moments], (layers, chips), (count - 2, far)))
        left_a, right_b, late_a, late_b, results = hold((left_a, right_b, late_a, late_b, results))
        far_a, far_b = hop(left_a, 1), hop(right_b, -1)
        over = [across(x) for x in (left_a, right_b, left_b, right_a)]
        over_late = across(late_a), across(late_b)
        near = [(0, own_a, 0, 0, 0), (0, own_b, 0, 0, down), (0, pair, 0, 1, 0), (0, left_a, back, 0, 0), (0, right_b, 1, 0, down)]
        near += [(0, left_b, back, 0, down), (0, right_a, 1, 0, 0), (1, late_a, far, 0, 0), (1, late_b, far, 0, far_rows)]
        whole, results[count - 2] = put([jax.ShapeDtypeStruct(weights[-1].shape, bf16), results[count - 2]], near)
        over, over_late, whole, results = hold((over, over_late, whole, results))
        near = [(0, over[0], back, 1, 0), (0, over[1], 1, 1, down), (0, over[2], back, 1, down), (0, over[3], 1, 1, 0)]
        near += [(1, over_late[0], far, 1, 0), (1, over_late[1], far, 1, far_rows)]
        whole, results[count - 2] = put([whole, results[count - 2]], near)
        far_a, far_b, whole = hold((far_a, far_b, whole))
        over_far_a, over_far_b = across(far_a), across(far_b)
        [whole] = put([whole], [(0, far_a, far, 0, 0), (0, far_b, far, 0, down)])
        over_far_a, over_far_b, whole = hold((over_far_a, over_far_b, whole))
        [whole] = put([whole], [(0, over_far_a, far, 1, 0), (0, over_far_b, far, 1, down)])
        return (*results[: count - 1], whole, *results[count - 1 :])

    all_of, cut = P(None, None, None), P(None, "dp", None)
    return jax.shard_map(
        step,
        mesh=mesh,
        in_specs=(P(("rep", "dp"), None, None, None),) * 3 + (all_of,) * 3 + (cut,) * 6,
        out_specs=(P("rep", None, None),) * 3 + (P("rep", "dp", None),) * 6,
        check_vma=False,
    )
```

```python
import functools
import itertools

import jax
import jax.numpy as jnp
from jax import lax
from jax.experimental import pallas as pl
from jax.experimental.pallas import tpu as pltpu
from jax.sharding import PartitionSpec as P


MESH = pl.DeviceIdType.MESH
CORES = 2
STRIP = 16
SLOTS = 6
VMEM = 67043328
LEAD = 0
SETS = 3


def f32(x):
    return x.astype(jnp.float32)


def strips(rows, body):
    def one(i, carry):
        body(pl.ds(pl.multiple_of(i * STRIP, STRIP), STRIP))
        return carry

    lax.fori_loop(0, rows // STRIP, one, None)


def kernel(chips, layers, kinds, *refs):
    count = len(kinds)
    last = count - 1
    take = iter(refs)
    g, w, m, v = ([next(take) for _ in range(count)] for _ in range(4))
    w_out = [next(take) for _ in range(last)]
    new_half, new_pair, far_half = [next(take) for _ in range(2)], next(take), [next(take) for _ in range(2)]
    m_out, v_out, part, arrived = ([next(take) for _ in range(count)] for _ in range(4))
    shapes = max(kinds) + 1
    own, m_set, v_set, w_set = ([next(take) for _ in range(shapes)] for _ in range(4))
    own_sem, set_in, set_out, pair_send, pair_recv, ring_send, ring_recv, gather_send, gather_recv, local_sem, early_pair_send, early_pair_recv, early_ring_send, early_ring_recv, turn_sem = take

    me = lax.axis_index("dp")
    chip, core = me // CORES, me % CORES
    partner = chip * CORES + (1 - core)
    turn = [lax.rem(chip + d, chips) for d in range(chips)]
    right, left = turn[1] * CORES + core, turn[chips - 1] * CORES + core
    far = chips // 2

    chunks = [(a, layer) for a in range(count) for layer in range(layers)]
    rows = [r.shape[2] for r in part]
    half = [r // 2 for r in rows]

    def remote(src, dst, send, recv, to):
        return pltpu.make_async_remote_copy(src_ref=src, dst_ref=dst, send_sem=send, recv_sem=recv, device_id={"dp": to}, device_id_type=MESH)

    waits = []

    def finish_later(copy, *ends):
        copy.start()
        waits.extend(getattr(copy, end) for end in ends)

    order = ((far, 0), (far, 1), (1, 1), (chips - 1, 0), (1, 0), (chips - 1, 1), (0, 0), (0, 1))

    def pieces(j, d, h):
        size = half[chunks[j][0]]
        if j == 0 and d == far:
            return [(n, h * size + n * STRIP, STRIP) for n in range(size // STRIP)]
        return [(None, h * size, size)]

    def pair_copy(j, d, h, piece):
        a, layer = chunks[j]
        n, row, size = piece
        src = g[a].at[0, layer, pl.ds(pl.multiple_of((turn[d] * CORES + 1 - core) * rows[a] + row, STRIP), size)]
        s = j * len(order) + order.index((d, h))
        sems = (pair_send.at[s], pair_recv.at[s]) if n is None else (early_pair_send.at[h, n], early_pair_recv.at[h, n])
        return remote(src, part[a].at[layer, d, pl.ds(row, size)], *sems, partner)

    def start_pair(j):
        copies = [[(d, h, piece) for piece in pieces(j, d, h)] for d, h in order]
        for together in [*zip(*copies[:2], strict=True), *copies[2:]]:
            for one in together:
                finish_later(pair_copy(j, *one), "wait_send")

    total = len(chunks)
    gathered = [j for j in range(total) if chunks[j][0] != last]
    plan = [("pair", 0), ("follow", 0)]
    for s in range(total):
        plan += [("first", s)]
        plan += [("pair", s + 1)] if s + 1 < total else []
        plan += [("lead", s)] if s == 0 else []
        plan += [("middle", s - 1)] if s >= 1 else []
        plan += [("middle", s)] if s == total - 1 else []
        plan += [("final", s - 2)] if s >= 2 else []
        plan += [("pass", s - 4)] if s >= 4 else []
        plan += [("hand", s - 5)] if s >= 5 else []
    passed = [j for act, j in plan if act == "pass"]
    handed = [j for act, j in plan if act == "hand"]
    rest = [j for j in gathered if j not in passed]
    plan += [("pass", rest[0]), ("final", total - 2)]
    plan += [("pass", j) for j in rest[1:]] + [("final", total - 1)]
    plan += [("hand", j) for j in gathered if j not in handed]

    uses = []
    for act, j in plan:
        uses += [(j, d, h) for d, h in {"first": order[:4], "middle": order[4:6], "final": order[6:]}.get(act, ())]
    of_kind = [[u for u in uses if kinds[chunks[u[0]][0]] == q] for q in range(shapes)]

    def own_copy(q, i):
        j, d, h = of_kind[q][i]
        a, layer = chunks[j]
        src = g[a].at[0, layer, pl.ds(pl.multiple_of((turn[d] * CORES + core) * rows[a] + h * half[a], STRIP), half[a])]
        return pltpu.make_async_copy(src, own[q].at[i % SLOTS], own_sem.at[q, i % SLOTS])

    for q in range(shapes):
        for i in range(min(SLOTS, len(of_kind[q]))):
            own_copy(q, i).start()
    used = [0] * shapes

    def add_own(j, d, h, extra, finish=None):
        a, layer = chunks[j]
        q = kinds[a]
        i = used[q]
        used[q] += 1
        assert of_kind[q][i] == (j, d, h)
        own_copy(q, i).wait()
        mine = own[q].at[i % SLOTS]
        total = part[a].at[layer, d, pl.ds(h * half[a], half[a])]

        def body(strip):
            x = f32(total[strip, :]) + f32(mine[strip, :])
            for one in extra:
                x = x + f32(one[strip, :])
            x = x.astype(jnp.bfloat16)
            total[strip, :] = x if finish is None else finish(strip, f32(x))

        for piece in pieces(j, d, h):
            pair_copy(j, d, h, piece).wait_recv()
            if piece[0] is None:
                strips(half[a], body)
            else:
                body(pl.ds(piece[1] - h * half[a], piece[2]))
                yield piece
        if i + SLOTS < len(of_kind[q]):
            own_copy(q, i + SLOTS).start()

    def do(work):
        for _ in work:
            pass

    ring_slots = ((far, 0), (1, 1), (1, 0), (far, 1), (chips - 1, 0), (chips - 1, 1))

    def ring_copy(j, slot, piece):
        a, layer = chunks[j]
        n, row, size = piece
        d, h = ring_slots[slot]
        src = part[a].at[layer, d, pl.ds(row, size)]
        dst = arrived[a].at[layer, slot, pl.ds(row - h * half[a], size)]
        s = j * 6 + slot
        sems = (ring_send.at[s], ring_recv.at[s]) if n is None else (early_ring_send.at[h, n], early_ring_recv.at[h, n])
        return remote(src, dst, *sems, right if slot < 3 else left)

    def send(j, slot):
        for piece in pieces(j, *ring_slots[slot]):
            finish_later(ring_copy(j, slot, piece), "wait_send")

    come = set()

    def arrival(j, slot):
        for piece in [] if (j, slot) in come else pieces(j, *ring_slots[slot]):
            ring_copy(j, slot, piece).wait_recv()
        come.add((j, slot))
        a, layer = chunks[j]
        return arrived[a].at[layer, slot]

    def follow(j):
        @pl.when(core == 1)
        def _():
            pl.semaphore_wait(turn_sem, 1)

    def lead(j):
        arrival(j, LEAD)

        @pl.when(core == 0)
        def _():
            pl.semaphore_signal(turn_sem, inc=1, device_id={"dp": partner}, device_id_type=MESH)

    def add_and_send(j, slot, extra=()):
        do(add_own(j, *ring_slots[slot], extra))
        send(j, slot)

    def first(j):
        if pieces(j, far, 0)[0][0] is None:
            add_and_send(j, 0)
            add_and_send(j, 3)
        else:
            for both in itertools.zip_longest(add_own(j, far, 0, ()), add_own(j, far, 1, ())):
                for slot, piece in zip((0, 3), both, strict=True):
                    finish_later(ring_copy(j, slot, piece), "wait_send")
        add_and_send(j, 1)
        add_and_send(j, 4)

    def middle(j):
        add_and_send(j, 2, (arrival(j, 0),))
        add_and_send(j, 5, (arrival(j, 3),))

    units = [[(j, h) for j in range(len(chunks)) for h in range(2) if kinds[chunks[j][0]] == q] for q in range(shapes)]

    def set_copies(q, i):
        j, h = units[q][i]
        a, layer = chunks[j]
        cut = pl.ds(h * half[a], half[a])
        mine = pl.ds(pl.multiple_of(me * rows[a] + h * half[a], STRIP), half[a])
        t = i % SETS
        return [
            pltpu.make_async_copy(m[a].at[layer, cut], m_set[q].at[t], set_in.at[q, t, 0]),
            pltpu.make_async_copy(v[a].at[layer, cut], v_set[q].at[t], set_in.at[q, t, 1]),
            pltpu.make_async_copy(w[a].at[layer, mine], w_set[q].at[t], set_in.at[q, t, 2]),
        ], [
            pltpu.make_async_copy(m_set[q].at[t], m_out[a].at[layer, cut], set_out.at[q, t, 0]),
            pltpu.make_async_copy(v_set[q].at[t], v_out[a].at[layer, cut], set_out.at[q, t, 1]),
        ]

    def start_set(q, i):
        if i < len(units[q]):
            if i >= SETS:
                for copy in set_copies(q, i - SETS)[1]:
                    copy.wait()
            for copy in set_copies(q, i)[0]:
                copy.start()

    for q in range(shapes):
        for i in range(SETS - 1):
            start_set(q, i)

    def update(j, h, extra):
        a, _ = chunks[j]
        q = kinds[a]
        i = units[q].index((j, h))
        ins, outs = set_copies(q, i)
        for copy in ins:
            copy.wait()
        mm, vv, ww = (s[q].at[i % SETS] for s in (m_set, v_set, w_set))

        def finish(strip, grad):
            old = f32(ww[strip, :])
            new_m = 0.9 * mm[strip, :] + 0.1 * grad
            new_v = 0.95 * vv[strip, :] + 0.05 * grad * grad
            mm[strip, :] = new_m
            vv[strip, :] = new_v
            step = new_m * lax.rsqrt(new_v + 1e-8) + 0.1 * old
            return (old - 0.02 * step).astype(jnp.bfloat16)

        do(add_own(j, 0, h, extra, finish))
        for copy in outs:
            copy.start()
        start_set(q, i + SETS - 1)

    def block(a, layer, chip_of, core_of, h=None):
        base = (chip_of * CORES + core_of) * rows[a]
        if h is None:
            return w_out[a].at[layer, pl.ds(pl.multiple_of(base, STRIP), rows[a])]
        return w_out[a].at[layer, pl.ds(pl.multiple_of(base + h * half[a], STRIP), half[a])]

    def gather_copy(j, n):
        a, layer = chunks[j]
        s = (gather_send.at[j, n], gather_recv.at[j, n])
        mine = lambda h: part[a].at[layer, 0, pl.ds(h * half[a], half[a])]
        if n < 4:
            h, to = n % 2, right if n < 2 else left
            return remote(mine(h), block(a, layer, chip, core, h), *s, to)
        if n < 6:
            d, h, to = ((chips - 1, 0, right), (1, 1, left))[n - 4]
            there = block(a, layer, turn[d], core, h)
            return remote(there, far_half[h].at[layer] if a == last - 1 else there, *s, to)
        if n == 6:
            return remote(part[a].at[layer, 0], block(a, layer, chip, core), *s, partner)
        d, h = ((chips - 1, None), (1, None), (far, 0), (far, 1))[n - 7]
        there = block(a, layer, turn[d], core, h)
        return remote(there, there, *s, partner)

    def go(j, n):
        finish_later(gather_copy(j, n), "wait_send", *(("wait_recv",) if n >= 6 else ()))

    def final(j):
        a, layer = chunks[j]
        if a == last:
            for h, slots in enumerate(((2, 4), (1, 5))):
                update(j, h, [arrival(j, slot) for slot in slots])
                half_of = part[a].at[layer, 0, pl.ds(h * half[a], half[a])]
                finish_later(pltpu.make_async_copy(half_of, new_half[h].at[layer], local_sem.at[j, h]), "wait")
            pair = remote(part[a].at[layer, 0], new_pair.at[layer], gather_send.at[j, 6], gather_recv.at[j, 6], partner)
            finish_later(pair, "wait_send", "wait_recv")
            return
        update(j, 0, (arrival(j, 2), arrival(j, 4)))
        go(j, 0)
        update(j, 1, (arrival(j, 1), arrival(j, 5)))
        go(j, 3)
        go(j, 1)
        go(j, 2)
        go(j, 6)
        finish_later(pltpu.make_async_copy(part[a].at[layer, 0], block(a, layer, chip, core), local_sem.at[j, 0]), "wait")

    def pass_on(j):
        gather_copy(j, 0).wait_recv()
        go(j, 4)
        gather_copy(j, 3).wait_recv()
        go(j, 5)
        gather_copy(j, 1).wait_recv()
        go(j, 7)
        gather_copy(j, 2).wait_recv()
        go(j, 8)

    def hand_over(j):
        for n, then in ((4, 9), (5, 10)):
            gather_copy(j, n).wait_recv()
            if chunks[j][0] != last - 1:
                go(j, then)

    barrier = pltpu.get_barrier_semaphore()
    for other in (partner, right, left):
        pl.semaphore_signal(barrier, inc=1, device_id={"dp": other}, device_id_type=MESH)
    pl.semaphore_wait(barrier, 3)

    acts = {"pair": start_pair, "follow": follow, "lead": lead, "first": first, "middle": middle, "final": final, "pass": pass_on, "hand": hand_over}
    for act, j in plan:
        acts[act](j)

    for q in range(shapes):
        for i in range(max(0, len(units[q]) - SETS), len(units[q])):
            for copy in set_copies(q, i)[1]:
                copy.wait()
    for wait in waits:
        wait()


def relayed(targets, pieces, near=(), leave=VMEM * 3 // 4):
    near = {id(x) for x in near}
    arrays = list({id(p[1]): p[1] for p in pieces}.values())
    at = {id(x): n for n, x in enumerate(arrays)}
    intos = [(n, t) for n, t in enumerate(targets) if not isinstance(t, jax.ShapeDtypeStruct)]
    through, direct = ([p for p in pieces if (id(p[1]) in near) == one] for one in (False, True))

    def body(*refs):
        take = iter(refs[len(intos) :])
        srcs, dsts, bufs = ([next(take) for _ in one] for one in (arrays, targets, through))
        sems = next(take)
        me = lax.axis_index("dp")
        place = me // CORES, me % CORES
        ins, outs = [], []
        for n, (t, x, _, here, there) in enumerate(through):
            ins.append(pltpu.make_async_copy(srcs[at[id(x)]].at[here(*place)], bufs[n], sems.at[n, 0]))
            outs.append(pltpu.make_async_copy(bufs[n], dsts[t].at[there(*place)], sems.at[n, 1]))
        for copy in ins:
            copy.start()
        for n, (t, x, _, here, there) in enumerate(direct):
            copy = pltpu.make_async_copy(srcs[at[id(x)]].at[here(*place)], dsts[t].at[there(*place)], sems.at[len(through) + n, 1])
            copy.start()
            outs.append(copy)
        for come, go in zip(ins, outs, strict=False):
            come.wait()
            go.start()
        for copy in outs:
            copy.wait()

    any_space = pl.BlockSpec(memory_space=pltpu.HBM)
    return pl.pallas_call(
        body,
        out_shape=[jax.ShapeDtypeStruct(t.shape, t.dtype) for t in targets],
        in_specs=[any_space] * len(intos) + [pl.BlockSpec(memory_space=pltpu.VMEM) if id(x) in near else any_space for x in arrays],
        out_specs=[any_space] * len(targets),
        scratch_shapes=[pltpu.VMEM(shape, x.dtype) for _, x, shape, *_ in through] + [pltpu.SemaphoreType.DMA((len(pieces), 2))],
        input_output_aliases={i: n for i, (n, _) in enumerate(intos)},
        compiler_params=pltpu.CompilerParams(vmem_limit_bytes=VMEM - leave),
    )(*[t for _, t in intos], *arrays)


def moved(arrays, steps, hole):
    def body(*refs):
        for src, dst in zip(refs[: len(arrays)], refs[len(arrays) :], strict=True):
            dst[...] = src[...]

    def spec(n, x):
        def at(i, j):
            if n != hole[0]:
                return i, j, 0
            step = jnp.where(j == hole[1], j - 1, j)
            return i, lax.rem(lax.axis_index("dp") // CORES + step, steps[1]), 0

        return pl.BlockSpec((x.shape[0] // steps[0], x.shape[1] // steps[1], x.shape[2]), at)

    specs = [spec(n, x) for n, x in enumerate(arrays)]
    return pl.pallas_call(
        body,
        out_shape=[jax.ShapeDtypeStruct(x.shape, x.dtype) for x in arrays],
        grid=steps,
        in_specs=specs,
        out_specs=specs,
        compiler_params=pltpu.CompilerParams(vmem_limit_bytes=VMEM),
    )(*arrays)


def placed(chips, targets, blocks, **options):
    def piece(t, x, d, other, first):
        rows = targets[t].shape[1] // (chips * CORES)

        def there(chip, core):
            base = (lax.rem(chip + d, chips) * CORES + (1 - core if other else core)) * rows + first
            return (slice(None), pl.ds(pl.multiple_of(base, STRIP), x.shape[1]))

        return (t, x, x.shape, lambda chip, core: slice(None), there)

    return relayed(targets, [piece(*one) for one in blocks], **options)


def solution(mesh):
    devices = mesh.shape["dp"]
    chips = devices // CORES

    def hop(x, d):
        return lax.ppermute(x, "dp", [(i, (i + d * CORES) % devices) for i in range(devices)])

    def across(x):
        return lax.ppermute(x, "dp", [(i, i // CORES * CORES + 1 - i % CORES) for i in range(devices)])

    def step(*arrays):
        terms, weights, m, v = (arrays[i : i + 3] for i in (0, 3, 6, 9))
        count, layers = len(weights), weights[0].shape[0]
        blocks = [one.shape[1:] for one in m]
        distinct = list(dict.fromkeys(blocks))
        kinds = tuple(distinct.index(b) for b in blocks)
        chunks = count * layers
        any_space = pl.BlockSpec(memory_space=pl.ANY)
        bf16 = jnp.bfloat16
        halves = [(b[0] // 2, b[1]) for b in distinct]
        cut_rows = blocks[-1][0] // 2
        dma = pltpu.SemaphoreType.DMA
        cut_cols, (far_rows, far_cols) = blocks[-1][1], (blocks[-2][0] // 2, blocks[-2][1])
        tail = [(layers, cut_rows, cut_cols)] * 2 + [(layers, *blocks[-1])] + [(layers, far_rows, far_cols)] * 2
        early = (2, blocks[0][0] // 2 // STRIP)
        out = pl.pallas_call(
            functools.partial(kernel, chips, layers, kinds),
            out_shape=[jax.ShapeDtypeStruct(one.shape, one.dtype) for one in weights[:-1]]
            + [jax.ShapeDtypeStruct(one, bf16) for one in tail]
            + [jax.ShapeDtypeStruct(one.shape, one.dtype) for one in (*m, *v)],
            in_specs=[any_space] * 4 * count,
            out_specs=[any_space] * (3 * count - 1 + len(tail)),
            scratch_shapes=[pltpu.VMEM((layers, chips, *b), bf16) for b in blocks]
            + [pltpu.VMEM((layers, 6, b[0] // 2, b[1]), bf16) for b in blocks]
            + [pltpu.VMEM((SLOTS, *b), bf16) for b in halves]
            + [pltpu.VMEM((SETS, *b), jnp.float32) for b in halves] * 2
            + [pltpu.VMEM((SETS, *b), bf16) for b in halves]
            + [dma((len(distinct), SLOTS)), dma((len(distinct), SETS, 3)), dma((len(distinct), SETS, 2))]
            + [dma((chunks * 2 * chips,))] * 2
            + [dma((chunks * 6,))] * 2
            + [dma((chunks, 11))] * 2
            + [dma((chunks, 2))]
            + [dma(early)] * 4
            + [pltpu.SemaphoreType.REGULAR],
            compiler_params=pltpu.CompilerParams(collective_id=0, has_side_effects=True, vmem_limit_bytes=VMEM),
        )(*terms, *weights, *m, *v)
        new, (own_a, own_b, pair, late_a, late_b), moments = out[: count - 1], out[count - 1 : count - 1 + len(tail)], out[count - 1 + len(tail) :]
        far, hold = chips // 2, lax.optimization_barrier
        back, down = chips - 1, cut_rows
        put = functools.partial(placed, chips)
        left_a, right_b = hop(own_a, 1), hop(own_b, -1)
        left_b, right_a = hop(own_b, 1), hop(own_a, -1)
        results = list(moved([*new, *moments], (layers, chips), (count - 2, far)))
        left_a, right_b, late_a, late_b, results = hold((left_a, right_b, late_a, late_b, results))
        far_a, far_b = hop(left_a, 1), hop(right_b, -1)
        over = [across(x) for x in (left_a, right_b, left_b, right_a)]
        over_late = across(late_a), across(late_b)
        held = sum(x.size * x.dtype.itemsize for x in (*over, *over_late, far_a, far_b)) + 2**18
        near = [(0, own_a, 0, 0, 0), (0, own_b, 0, 0, down), (0, pair, 0, 1, 0), (0, left_a, back, 0, 0), (0, right_b, 1, 0, down)]
        near += [(0, left_b, back, 0, down), (0, right_a, 1, 0, 0), (1, late_a, far, 0, 0), (1, late_b, far, 0, far_rows)]
        whole, results[count - 2] = put([jax.ShapeDtypeStruct(weights[-1].shape, bf16), results[count - 2]], near, leave=held)
        over, over_late, whole, results = hold((over, over_late, whole, results))
        near = [(0, over[0], back, 1, 0), (0, over[1], 1, 1, down), (0, over[2], back, 1, down), (0, over[3], 1, 1, 0)]
        near += [(1, over_late[0], far, 1, 0), (1, over_late[1], far, 1, far_rows)]
        whole, results[count - 2] = put([whole, results[count - 2]], near, near=[*over, *over_late])
        far_a, far_b, whole = hold((far_a, far_b, whole))
        over_far_a, over_far_b = across(far_a), across(far_b)
        [whole] = put([whole], [(0, far_a, far, 0, 0), (0, far_b, far, 0, down)], near=[far_a, far_b])
        over_far_a, over_far_b, whole = hold((over_far_a, over_far_b, whole))
        [whole] = put([whole], [(0, over_far_a, far, 1, 0), (0, over_far_b, far, 1, down)], near=[over_far_a, over_far_b])
        return (*results[: count - 1], whole, *results[count - 1 :])

    all_of, cut = P(None, None, None), P(None, "dp", None)
    return jax.shard_map(
        step,
        mesh=mesh,
        in_specs=(P(("rep", "dp"), None, None, None),) * 3 + (all_of,) * 3 + (cut,) * 6,
        out_specs=(P("rep", None, None),) * 3 + (P("rep", "dp", None),) * 6,
        check_vma=False,
    )
```

```python
import functools
import itertools

import jax
import jax.numpy as jnp
from jax import lax
from jax.experimental import pallas as pl
from jax.experimental.pallas import tpu as pltpu
from jax.sharding import PartitionSpec as P


MESH = pl.DeviceIdType.MESH
CORES = 2
STRIP = 16
SLOTS = 6
VMEM = 67043328
LEAD = 0
SETS = 3


def f32(x):
    return x.astype(jnp.float32)


def strips(rows, body):
    def one(i, carry):
        body(pl.ds(pl.multiple_of(i * STRIP, STRIP), STRIP))
        return carry

    lax.fori_loop(0, rows // STRIP, one, None)


def kernel(chips, layers, kinds, *refs):
    count = len(kinds)
    last = count - 1
    take = iter(refs)
    g, w, m, v = ([next(take) for _ in range(count)] for _ in range(4))
    w_out = [next(take) for _ in range(last)]
    new_half, new_pair, far_half = [next(take) for _ in range(2)], next(take), [next(take) for _ in range(2)]
    m_out, v_out, part, arrived = ([next(take) for _ in range(count)] for _ in range(4))
    shapes = max(kinds) + 1
    own, m_set, v_set, w_set = ([next(take) for _ in range(shapes)] for _ in range(4))
    own_sem, set_in, set_out, pair_send, pair_recv, ring_send, ring_recv, gather_send, gather_recv, local_sem, early_pair_send, early_pair_recv, early_ring_send, early_ring_recv, turn_sem = take

    me = lax.axis_index("dp")
    chip, core = me // CORES, me % CORES
    partner = chip * CORES + (1 - core)
    turn = [lax.rem(chip + d, chips) for d in range(chips)]
    right, left = turn[1] * CORES + core, turn[chips - 1] * CORES + core
    far = chips // 2

    barrier = pltpu.get_barrier_semaphore()
    for other in (left, right, partner):
        pl.semaphore_signal(barrier, inc=1, device_id={"dp": other}, device_id_type=MESH)

    chunks = [(a, layer) for a in range(count) for layer in range(layers)]
    rows = [r.shape[2] for r in part]
    half = [r // 2 for r in rows]

    def remote(src, dst, send, recv, to):
        return pltpu.make_async_remote_copy(src_ref=src, dst_ref=dst, send_sem=send, recv_sem=recv, device_id={"dp": to}, device_id_type=MESH)

    waits = []

    def finish_later(copy, *ends):
        copy.start()
        waits.extend(getattr(copy, end) for end in ends)

    order = ((far, 0), (far, 1), (1, 1), (chips - 1, 0), (1, 0), (chips - 1, 1), (0, 0), (0, 1))

    def pieces(j, d, h):
        size = half[chunks[j][0]]
        if j == 0 and d == far:
            return [(n, h * size + n * STRIP, STRIP) for n in range(size // STRIP)]
        return [(None, h * size, size)]

    def pair_copy(j, d, h, piece):
        a, layer = chunks[j]
        n, row, size = piece
        src = g[a].at[0, layer, pl.ds(pl.multiple_of((turn[d] * CORES + 1 - core) * rows[a] + row, STRIP), size)]
        s = j * len(order) + order.index((d, h))
        sems = (pair_send.at[s], pair_recv.at[s]) if n is None else (early_pair_send.at[h, n], early_pair_recv.at[h, n])
        return remote(src, part[a].at[layer, d, pl.ds(row, size)], *sems, partner)

    def start_pair(j):
        copies = [[(d, h, piece) for piece in pieces(j, d, h)] for d, h in order]
        for together in [*zip(*copies[:2], strict=True), *copies[2:]]:
            for one in together:
                finish_later(pair_copy(j, *one), "wait_send")

    total = len(chunks)
    gathered = [j for j in range(total) if chunks[j][0] != last]
    plan = [("pair", 0), ("follow", 0)]
    for s in range(total):
        plan += [("first", s)]
        plan += [("pair", s + 1)] if s + 1 < total else []
        plan += [("lead", s)] if s == 0 else []
        plan += [("middle", s - 1)] if s >= 1 else []
        plan += [("middle", s)] if s == total - 1 else []
        plan += [("final", s - 2)] if s >= 2 else []
        plan += [("pass", s - 4)] if s >= 4 else []
        plan += [("hand", s - 5)] if s >= 5 else []
    passed = [j for act, j in plan if act == "pass"]
    handed = [j for act, j in plan if act == "hand"]
    rest = [j for j in gathered if j not in passed]
    plan += [("pass", rest[0]), ("final", total - 2)]
    plan += [("pass", j) for j in rest[1:]] + [("final", total - 1)]
    plan += [("hand", j) for j in gathered if j not in handed]

    uses = []
    for act, j in plan:
        uses += [(j, d, h) for d, h in {"first": order[:4], "middle": order[4:6], "final": order[6:]}.get(act, ())]
    of_kind = [[u for u in uses if kinds[chunks[u[0]][0]] == q] for q in range(shapes)]

    def own_copy(q, i):
        j, d, h = of_kind[q][i]
        a, layer = chunks[j]
        src = g[a].at[0, layer, pl.ds(pl.multiple_of((turn[d] * CORES + core) * rows[a] + h * half[a], STRIP), half[a])]
        return pltpu.make_async_copy(src, own[q].at[i % SLOTS], own_sem.at[q, i % SLOTS])

    for q in range(shapes):
        for i in range(min(SLOTS, len(of_kind[q]))):
            own_copy(q, i).start()
    used = [0] * shapes

    def add_own(j, d, h, extra, finish=None):
        a, layer = chunks[j]
        q = kinds[a]
        i = used[q]
        used[q] += 1
        assert of_kind[q][i] == (j, d, h)
        own_copy(q, i).wait()
        mine = own[q].at[i % SLOTS]
        total = part[a].at[layer, d, pl.ds(h * half[a], half[a])]

        def body(strip):
            x = f32(total[strip, :]) + f32(mine[strip, :])
            for one in extra:
                x = x + f32(one[strip, :])
            x = x.astype(jnp.bfloat16)
            total[strip, :] = x if finish is None else finish(strip, f32(x))

        for piece in pieces(j, d, h):
            pair_copy(j, d, h, piece).wait_recv()
            if piece[0] is None:
                strips(half[a], body)
            else:
                body(pl.ds(piece[1] - h * half[a], piece[2]))
                yield piece
        if i + SLOTS < len(of_kind[q]):
            own_copy(q, i + SLOTS).start()

    def do(work):
        for _ in work:
            pass

    ring_slots = ((far, 0), (1, 1), (1, 0), (far, 1), (chips - 1, 0), (chips - 1, 1))

    def ring_copy(j, slot, piece):
        a, layer = chunks[j]
        n, row, size = piece
        d, h = ring_slots[slot]
        src = part[a].at[layer, d, pl.ds(row, size)]
        dst = arrived[a].at[layer, slot, pl.ds(row - h * half[a], size)]
        s = j * 6 + slot
        sems = (ring_send.at[s], ring_recv.at[s]) if n is None else (early_ring_send.at[h, n], early_ring_recv.at[h, n])
        return remote(src, dst, *sems, right if slot < 3 else left)

    def send(j, slot):
        for piece in pieces(j, *ring_slots[slot]):
            finish_later(ring_copy(j, slot, piece), "wait_send")

    come = set()

    def arrival(j, slot):
        for piece in [] if (j, slot) in come else pieces(j, *ring_slots[slot]):
            ring_copy(j, slot, piece).wait_recv()
        come.add((j, slot))
        a, layer = chunks[j]
        return arrived[a].at[layer, slot]

    def follow(j):
        @pl.when(core == 1)
        def _():
            pl.semaphore_wait(turn_sem, 1)

    def lead(j):
        arrival(j, LEAD)

        @pl.when(core == 0)
        def _():
            pl.semaphore_signal(turn_sem, inc=1, device_id={"dp": partner}, device_id_type=MESH)

    def add_and_send(j, slot, extra=()):
        do(add_own(j, *ring_slots[slot], extra))
        send(j, slot)

    def first(j):
        if pieces(j, far, 0)[0][0] is None:
            add_and_send(j, 0)
            add_and_send(j, 3)
        else:
            for both in itertools.zip_longest(add_own(j, far, 0, ()), add_own(j, far, 1, ())):
                for slot, piece in zip((0, 3), both, strict=True):
                    finish_later(ring_copy(j, slot, piece), "wait_send")
        add_and_send(j, 1)
        add_and_send(j, 4)

    def middle(j):
        add_and_send(j, 2, (arrival(j, 0),))
        add_and_send(j, 5, (arrival(j, 3),))

    units = [[(j, h) for j in range(len(chunks)) for h in range(2) if kinds[chunks[j][0]] == q] for q in range(shapes)]

    def set_copies(q, i):
        j, h = units[q][i]
        a, layer = chunks[j]
        cut = pl.ds(h * half[a], half[a])
        mine = pl.ds(pl.multiple_of(me * rows[a] + h * half[a], STRIP), half[a])
        t = i % SETS
        return [
            pltpu.make_async_copy(m[a].at[layer, cut], m_set[q].at[t], set_in.at[q, t, 0]),
            pltpu.make_async_copy(v[a].at[layer, cut], v_set[q].at[t], set_in.at[q, t, 1]),
            pltpu.make_async_copy(w[a].at[layer, mine], w_set[q].at[t], set_in.at[q, t, 2]),
        ], [
            pltpu.make_async_copy(m_set[q].at[t], m_out[a].at[layer, cut], set_out.at[q, t, 0]),
            pltpu.make_async_copy(v_set[q].at[t], v_out[a].at[layer, cut], set_out.at[q, t, 1]),
        ]

    def start_set(q, i):
        if i < len(units[q]):
            if i >= SETS:
                for copy in set_copies(q, i - SETS)[1]:
                    copy.wait()
            for copy in set_copies(q, i)[0]:
                copy.start()

    for q in range(shapes):
        for i in range(SETS - 1):
            start_set(q, i)

    def update(j, h, extra):
        a, _ = chunks[j]
        q = kinds[a]
        i = units[q].index((j, h))
        ins, outs = set_copies(q, i)
        for copy in ins:
            copy.wait()
        mm, vv, ww = (s[q].at[i % SETS] for s in (m_set, v_set, w_set))

        def finish(strip, grad):
            old = f32(ww[strip, :])
            new_m = 0.9 * mm[strip, :] + 0.1 * grad
            new_v = 0.95 * vv[strip, :] + 0.05 * grad * grad
            mm[strip, :] = new_m
            vv[strip, :] = new_v
            step = new_m * lax.rsqrt(new_v + 1e-8) + 0.1 * old
            return (old - 0.02 * step).astype(jnp.bfloat16)

        do(add_own(j, 0, h, extra, finish))
        for copy in outs:
            copy.start()
        start_set(q, i + SETS - 1)

    def block(a, layer, chip_of, core_of, h=None):
        base = (chip_of * CORES + core_of) * rows[a]
        if h is None:
            return w_out[a].at[layer, pl.ds(pl.multiple_of(base, STRIP), rows[a])]
        return w_out[a].at[layer, pl.ds(pl.multiple_of(base + h * half[a], STRIP), half[a])]

    def gather_copy(j, n):
        a, layer = chunks[j]
        s = (gather_send.at[j, n], gather_recv.at[j, n])
        mine = lambda h: part[a].at[layer, 0, pl.ds(h * half[a], half[a])]
        if n < 4:
            h, to = n % 2, right if n < 2 else left
            return remote(mine(h), block(a, layer, chip, core, h), *s, to)
        if n < 6:
            d, h, to = ((chips - 1, 0, right), (1, 1, left))[n - 4]
            there = block(a, layer, turn[d], core, h)
            return remote(there, far_half[h].at[layer] if a == last - 1 else there, *s, to)
        if n == 6:
            return remote(part[a].at[layer, 0], block(a, layer, chip, core), *s, partner)
        d, h = ((chips - 1, None), (1, None), (far, 0), (far, 1))[n - 7]
        there = block(a, layer, turn[d], core, h)
        return remote(there, there, *s, partner)

    def go(j, n):
        finish_later(gather_copy(j, n), "wait_send", *(("wait_recv",) if n >= 6 else ()))

    def final(j):
        a, layer = chunks[j]
        if a == last:
            for h, slots in enumerate(((2, 4), (1, 5))):
                update(j, h, [arrival(j, slot) for slot in slots])
                half_of = part[a].at[layer, 0, pl.ds(h * half[a], half[a])]
                finish_later(pltpu.make_async_copy(half_of, new_half[h].at[layer], local_sem.at[j, h]), "wait")
            pair = remote(part[a].at[layer, 0], new_pair.at[layer], gather_send.at[j, 6], gather_recv.at[j, 6], partner)
            finish_later(pair, "wait_send", "wait_recv")
            return
        update(j, 0, (arrival(j, 2), arrival(j, 4)))
        go(j, 0)
        update(j, 1, (arrival(j, 1), arrival(j, 5)))
        go(j, 3)
        go(j, 1)
        go(j, 2)
        go(j, 6)
        finish_later(pltpu.make_async_copy(part[a].at[layer, 0], block(a, layer, chip, core), local_sem.at[j, 0]), "wait")

    def pass_on(j):
        gather_copy(j, 0).wait_recv()
        go(j, 4)
        gather_copy(j, 3).wait_recv()
        go(j, 5)
        gather_copy(j, 1).wait_recv()
        go(j, 7)
        gather_copy(j, 2).wait_recv()
        go(j, 8)

    def hand_over(j):
        for n, then in ((4, 9), (5, 10)):
            gather_copy(j, n).wait_recv()
            if chunks[j][0] != last - 1:
                go(j, then)

    pl.semaphore_wait(barrier, 3)

    acts = {"pair": start_pair, "follow": follow, "lead": lead, "first": first, "middle": middle, "final": final, "pass": pass_on, "hand": hand_over}
    for act, j in plan:
        acts[act](j)

    for q in range(shapes):
        for i in range(max(0, len(units[q]) - SETS), len(units[q])):
            for copy in set_copies(q, i)[1]:
                copy.wait()
    for wait in waits:
        wait()


def relayed(targets, pieces, near=(), leave=VMEM * 3 // 4):
    near = {id(x) for x in near}
    arrays = list({id(p[1]): p[1] for p in pieces}.values())
    at = {id(x): n for n, x in enumerate(arrays)}
    intos = [(n, t) for n, t in enumerate(targets) if not isinstance(t, jax.ShapeDtypeStruct)]
    through, direct = ([p for p in pieces if (id(p[1]) in near) == one] for one in (False, True))

    def body(*refs):
        take = iter(refs[len(intos) :])
        srcs, dsts, bufs = ([next(take) for _ in one] for one in (arrays, targets, through))
        sems = next(take)
        me = lax.axis_index("dp")
        place = me // CORES, me % CORES
        ins, outs = [], []
        for n, (t, x, _, here, there) in enumerate(through):
            ins.append(pltpu.make_async_copy(srcs[at[id(x)]].at[here(*place)], bufs[n], sems.at[n, 0]))
            outs.append(pltpu.make_async_copy(bufs[n], dsts[t].at[there(*place)], sems.at[n, 1]))
        for copy in ins:
            copy.start()
        for n, (t, x, _, here, there) in enumerate(direct):
            copy = pltpu.make_async_copy(srcs[at[id(x)]].at[here(*place)], dsts[t].at[there(*place)], sems.at[len(through) + n, 1])
            copy.start()
            outs.append(copy)
        for come, go in zip(ins, outs, strict=False):
            come.wait()
            go.start()
        for copy in outs:
            copy.wait()

    any_space = pl.BlockSpec(memory_space=pltpu.HBM)
    return pl.pallas_call(
        body,
        out_shape=[jax.ShapeDtypeStruct(t.shape, t.dtype) for t in targets],
        in_specs=[any_space] * len(intos) + [pl.BlockSpec(memory_space=pltpu.VMEM) if id(x) in near else any_space for x in arrays],
        out_specs=[any_space] * len(targets),
        scratch_shapes=[pltpu.VMEM(shape, x.dtype) for _, x, shape, *_ in through] + [pltpu.SemaphoreType.DMA((len(pieces), 2))],
        input_output_aliases={i: n for i, (n, _) in enumerate(intos)},
        compiler_params=pltpu.CompilerParams(vmem_limit_bytes=VMEM - leave),
    )(*[t for _, t in intos], *arrays)


def moved(arrays, steps, hole):
    def body(*refs):
        for src, dst in zip(refs[: len(arrays)], refs[len(arrays) :], strict=True):
            dst[...] = src[...]

    def spec(n, x):
        def at(i, j):
            if n != hole[0]:
                return i, j, 0
            step = jnp.where(j == hole[1], j - 1, j)
            return i, lax.rem(lax.axis_index("dp") // CORES + step, steps[1]), 0

        return pl.BlockSpec((x.shape[0] // steps[0], x.shape[1] // steps[1], x.shape[2]), at)

    specs = [spec(n, x) for n, x in enumerate(arrays)]
    return pl.pallas_call(
        body,
        out_shape=[jax.ShapeDtypeStruct(x.shape, x.dtype) for x in arrays],
        grid=steps,
        in_specs=specs,
        out_specs=specs,
        compiler_params=pltpu.CompilerParams(vmem_limit_bytes=VMEM),
    )(*arrays)


def placed(chips, targets, blocks, **options):
    def piece(t, x, d, other, first):
        rows = targets[t].shape[1] // (chips * CORES)

        def there(chip, core):
            base = (lax.rem(chip + d, chips) * CORES + (1 - core if other else core)) * rows + first
            return (slice(None), pl.ds(pl.multiple_of(base, STRIP), x.shape[1]))

        return (t, x, x.shape, lambda chip, core: slice(None), there)

    return relayed(targets, [piece(*one) for one in blocks], **options)


def solution(mesh):
    devices = mesh.shape["dp"]
    chips = devices // CORES

    def hop(x, d):
        return lax.ppermute(x, "dp", [(i, (i + d * CORES) % devices) for i in range(devices)])

    def across(x):
        return lax.ppermute(x, "dp", [(i, i // CORES * CORES + 1 - i % CORES) for i in range(devices)])

    def step(*arrays):
        terms, weights, m, v = (arrays[i : i + 3] for i in (0, 3, 6, 9))
        count, layers = len(weights), weights[0].shape[0]
        blocks = [one.shape[1:] for one in m]
        distinct = list(dict.fromkeys(blocks))
        kinds = tuple(distinct.index(b) for b in blocks)
        chunks = count * layers
        any_space = pl.BlockSpec(memory_space=pl.ANY)
        bf16 = jnp.bfloat16
        halves = [(b[0] // 2, b[1]) for b in distinct]
        cut_rows = blocks[-1][0] // 2
        dma = pltpu.SemaphoreType.DMA
        cut_cols, (far_rows, far_cols) = blocks[-1][1], (blocks[-2][0] // 2, blocks[-2][1])
        tail = [(layers, cut_rows, cut_cols)] * 2 + [(layers, *blocks[-1])] + [(layers, far_rows, far_cols)] * 2
        early = (2, blocks[0][0] // 2 // STRIP)
        out = pl.pallas_call(
            functools.partial(kernel, chips, layers, kinds),
            out_shape=[jax.ShapeDtypeStruct(one.shape, one.dtype) for one in weights[:-1]]
            + [jax.ShapeDtypeStruct(one, bf16) for one in tail]
            + [jax.ShapeDtypeStruct(one.shape, one.dtype) for one in (*m, *v)],
            in_specs=[any_space] * 4 * count,
            out_specs=[any_space] * (3 * count - 1 + len(tail)),
            scratch_shapes=[pltpu.VMEM((layers, chips, *b), bf16) for b in blocks]
            + [pltpu.VMEM((layers, 6, b[0] // 2, b[1]), bf16) for b in blocks]
            + [pltpu.VMEM((SLOTS, *b), bf16) for b in halves]
            + [pltpu.VMEM((SETS, *b), jnp.float32) for b in halves] * 2
            + [pltpu.VMEM((SETS, *b), bf16) for b in halves]
            + [dma((len(distinct), SLOTS)), dma((len(distinct), SETS, 3)), dma((len(distinct), SETS, 2))]
            + [dma((chunks * 2 * chips,))] * 2
            + [dma((chunks * 6,))] * 2
            + [dma((chunks, 11))] * 2
            + [dma((chunks, 2))]
            + [dma(early)] * 4
            + [pltpu.SemaphoreType.REGULAR],
            compiler_params=pltpu.CompilerParams(collective_id=0, has_side_effects=True, vmem_limit_bytes=VMEM),
        )(*terms, *weights, *m, *v)
        new, (own_a, own_b, pair, late_a, late_b), moments = out[: count - 1], out[count - 1 : count - 1 + len(tail)], out[count - 1 + len(tail) :]
        far, hold = chips // 2, lax.optimization_barrier
        back, down = chips - 1, cut_rows
        put = functools.partial(placed, chips)
        left_a, right_b = hop(own_a, 1), hop(own_b, -1)
        left_b, right_a = hop(own_b, 1), hop(own_a, -1)
        results = list(moved([*new, *moments], (layers, chips), (count - 2, far)))
        left_a, right_b, late_a, late_b, results = hold((left_a, right_b, late_a, late_b, results))
        far_a, far_b = hop(left_a, 1), hop(right_b, -1)
        over = [across(x) for x in (left_a, right_b, left_b, right_a)]
        over_late = across(late_a), across(late_b)
        held = sum(x.size * x.dtype.itemsize for x in (*over, *over_late, far_a, far_b)) + 2**18
        near = [(0, own_a, 0, 0, 0), (0, own_b, 0, 0, down), (0, pair, 0, 1, 0), (0, left_a, back, 0, 0), (0, right_b, 1, 0, down)]
        near += [(0, left_b, back, 0, down), (0, right_a, 1, 0, 0), (1, late_a, far, 0, 0), (1, late_b, far, 0, far_rows)]
        whole, results[count - 2] = put([jax.ShapeDtypeStruct(weights[-1].shape, bf16), results[count - 2]], near, leave=held)
        over, over_late, whole, results = hold((over, over_late, whole, results))
        near = [(0, over[0], back, 1, 0), (0, over[1], 1, 1, down), (0, over[2], back, 1, down), (0, over[3], 1, 1, 0)]
        near += [(1, over_late[0], far, 1, 0), (1, over_late[1], far, 1, far_rows)]
        whole, results[count - 2] = put([whole, results[count - 2]], near, near=[*over, *over_late])
        far_a, whole = hold((far_a, whole))
        over_far_a = across(far_a)
        far_b, whole = hold((far_b, whole))
        over_far_b = across(far_b)
        [whole] = put([whole], [(0, far_a, far, 0, 0), (0, far_b, far, 0, down)], near=[far_a, far_b])
        over_far_a, whole = hold((over_far_a, whole))
        [whole] = put([whole], [(0, over_far_a, far, 1, 0)], near=[over_far_a])
        over_far_b, whole = hold((over_far_b, whole))
        [whole] = put([whole], [(0, over_far_b, far, 1, down)], near=[over_far_b])
        return (*results[: count - 1], whole, *results[count - 1 :])

    all_of, cut = P(None, None, None), P(None, "dp", None)
    return jax.shard_map(
        step,
        mesh=mesh,
        in_specs=(P(("rep", "dp"), None, None, None),) * 3 + (all_of,) * 3 + (cut,) * 6,
        out_specs=(P("rep", None, None),) * 3 + (P("rep", "dp", None),) * 6,
        check_vma=False,
    )
```

```python
import functools
import itertools

import jax
import jax.numpy as jnp
from jax import lax
from jax.experimental import pallas as pl
from jax.experimental.pallas import tpu as pltpu
from jax.sharding import PartitionSpec as P


MESH = pl.DeviceIdType.MESH
CORES = 2
STRIP = 16
SLOTS = 6
VMEM = 67043328
LEAD = 0
LAST = 16
SETS = 3


def f32(x):
    return x.astype(jnp.float32)


def strips(rows, body):
    def one(i, carry):
        body(pl.ds(pl.multiple_of(i * STRIP, STRIP), STRIP))
        return carry

    lax.fori_loop(0, rows // STRIP, one, None)


def kernel(chips, layers, kinds, *refs):
    count = len(kinds)
    last = count - 1
    take = iter(refs)
    g, w, m, v = ([next(take) for _ in range(count)] for _ in range(4))
    w_out = [next(take) for _ in range(last)]
    new_half, new_pair, far_half = [next(take) for _ in range(2)], next(take), [next(take) for _ in range(2)]
    to_pass = [next(take) for _ in range(2)]
    m_out, v_out, part, arrived = ([next(take) for _ in range(count)] for _ in range(4))
    shapes = max(kinds) + 1
    own, m_set, v_set, w_set = ([next(take) for _ in range(shapes)] for _ in range(4))
    own_sem, set_in, set_out, pair_send, pair_recv, ring_send, ring_recv, gather_send, gather_recv, local_sem, early_pair_send, early_pair_recv, early_ring_send, early_ring_recv, turn_sem, pass_sem = take

    me = lax.axis_index("dp")
    chip, core = me // CORES, me % CORES
    partner = chip * CORES + (1 - core)
    turn = [lax.rem(chip + d, chips) for d in range(chips)]
    right, left = turn[1] * CORES + core, turn[chips - 1] * CORES + core
    far = chips // 2

    barrier = pltpu.get_barrier_semaphore()
    for other in (left, right, partner):
        pl.semaphore_signal(barrier, inc=1, device_id={"dp": other}, device_id_type=MESH)

    chunks = [(a, layer) for a in range(count) for layer in range(layers)]
    rows = [r.shape[2] for r in part]
    half = [r // 2 for r in rows]

    def remote(src, dst, send, recv, to):
        return pltpu.make_async_remote_copy(src_ref=src, dst_ref=dst, send_sem=send, recv_sem=recv, device_id={"dp": to}, device_id_type=MESH)

    waits = []

    def finish_later(copy, *ends):
        copy.start()
        waits.extend(getattr(copy, end) for end in ends)

    order = ((far, 0), (far, 1), (1, 1), (chips - 1, 0), (1, 0), (chips - 1, 1), (0, 0), (0, 1))

    def pieces(j, d, h):
        size = half[chunks[j][0]]
        if j == 0 and d == far:
            return [(n, h * size + n * STRIP, STRIP) for n in range(size // STRIP)]
        return [(None, h * size, size)]

    def pair_copy(j, d, h, piece):
        a, layer = chunks[j]
        n, row, size = piece
        src = g[a].at[0, layer, pl.ds(pl.multiple_of((turn[d] * CORES + 1 - core) * rows[a] + row, STRIP), size)]
        s = j * len(order) + order.index((d, h))
        sems = (pair_send.at[s], pair_recv.at[s]) if n is None else (early_pair_send.at[h, n], early_pair_recv.at[h, n])
        return remote(src, part[a].at[layer, d, pl.ds(row, size)], *sems, partner)

    def start_pair(j):
        copies = [[(d, h, piece) for piece in pieces(j, d, h)] for d, h in order]
        for together in [*zip(*copies[:2], strict=True), *copies[2:]]:
            for one in together:
                finish_later(pair_copy(j, *one), "wait_send")

    total = len(chunks)
    gathered = [j for j in range(total) if chunks[j][0] != last]
    plan = [("pair", 0), ("follow", 0)]
    for s in range(total):
        plan += [("first", s)]
        plan += [("pair", s + 1)] if s + 1 < total else []
        plan += [("lead", s)] if s == 0 else []
        plan += [("middle", s - 1)] if s >= 1 else []
        plan += [("middle", s)] if s == total - 1 else []
        plan += [("final", s - 2)] if s >= 2 else []
        plan += [("pass", s - 4)] if s >= 4 else []
        plan += [("hand", s - 5)] if s >= 5 else []
    passed = [j for act, j in plan if act == "pass"]
    handed = [j for act, j in plan if act == "hand"]
    rest = [j for j in gathered if j not in passed]
    plan += [("pass", rest[0]), ("final", total - 2)]
    plan += [("pass", j) for j in rest[1:]] + [("final", total - 1)]
    plan += [("hand", j) for j in gathered if j not in handed]

    uses = []
    for act, j in plan:
        uses += [(j, d, h) for d, h in {"first": order[:4], "middle": order[4:6], "final": order[6:]}.get(act, ())]
    of_kind = [[u for u in uses if kinds[chunks[u[0]][0]] == q] for q in range(shapes)]

    def own_copy(q, i):
        j, d, h = of_kind[q][i]
        a, layer = chunks[j]
        src = g[a].at[0, layer, pl.ds(pl.multiple_of((turn[d] * CORES + core) * rows[a] + h * half[a], STRIP), half[a])]
        return pltpu.make_async_copy(src, own[q].at[i % SLOTS], own_sem.at[q, i % SLOTS])

    for q in range(shapes):
        for i in range(min(SLOTS, len(of_kind[q]))):
            own_copy(q, i).start()
    used = [0] * shapes

    def add_own(j, d, h, extra, finish=None):
        a, layer = chunks[j]
        q = kinds[a]
        i = used[q]
        used[q] += 1
        assert of_kind[q][i] == (j, d, h)
        own_copy(q, i).wait()
        mine = own[q].at[i % SLOTS]
        total = part[a].at[layer, d, pl.ds(h * half[a], half[a])]

        def body(strip):
            x = f32(total[strip, :]) + f32(mine[strip, :])
            for one in extra:
                x = x + f32(one[strip, :])
            x = x.astype(jnp.bfloat16)
            total[strip, :] = x if finish is None else finish(strip, f32(x))

        for piece in pieces(j, d, h):
            pair_copy(j, d, h, piece).wait_recv()
            if piece[0] is None:
                strips(half[a], body)
            else:
                body(pl.ds(piece[1] - h * half[a], piece[2]))
                yield piece
        if i + SLOTS < len(of_kind[q]):
            own_copy(q, i + SLOTS).start()

    def do(work):
        for _ in work:
            pass

    ring_slots = ((far, 0), (1, 1), (1, 0), (far, 1), (chips - 1, 0), (chips - 1, 1))

    def ring_copy(j, slot, piece):
        a, layer = chunks[j]
        n, row, size = piece
        d, h = ring_slots[slot]
        src = part[a].at[layer, d, pl.ds(row, size)]
        dst = arrived[a].at[layer, slot, pl.ds(row - h * half[a], size)]
        s = j * 6 + slot
        sems = (ring_send.at[s], ring_recv.at[s]) if n is None else (early_ring_send.at[h, n], early_ring_recv.at[h, n])
        return remote(src, dst, *sems, right if slot < 3 else left)

    def send(j, slot):
        for piece in pieces(j, *ring_slots[slot]):
            finish_later(ring_copy(j, slot, piece), "wait_send")

    come = set()

    def arrival(j, slot):
        for piece in [] if (j, slot) in come else pieces(j, *ring_slots[slot]):
            ring_copy(j, slot, piece).wait_recv()
        come.add((j, slot))
        a, layer = chunks[j]
        return arrived[a].at[layer, slot]

    def follow(j):
        @pl.when(core == 1)
        def _():
            pl.semaphore_wait(turn_sem, 1)

    def lead(j):
        arrival(j, LEAD)

        @pl.when(core == 0)
        def _():
            pl.semaphore_signal(turn_sem, inc=1, device_id={"dp": partner}, device_id_type=MESH)

    def add_and_send(j, slot, extra=()):
        do(add_own(j, *ring_slots[slot], extra))
        send(j, slot)

    def first(j):
        if pieces(j, far, 0)[0][0] is None:
            add_and_send(j, 0)
            add_and_send(j, 3)
        else:
            for both in itertools.zip_longest(add_own(j, far, 0, ()), add_own(j, far, 1, ())):
                for slot, piece in zip((0, 3), both, strict=True):
                    finish_later(ring_copy(j, slot, piece), "wait_send")
        add_and_send(j, 1)
        add_and_send(j, 4)

    def middle(j):
        add_and_send(j, 2, (arrival(j, 0),))
        add_and_send(j, 5, (arrival(j, 3),))

    units = [[(j, h) for j in range(len(chunks)) for h in range(2) if kinds[chunks[j][0]] == q] for q in range(shapes)]

    def set_copies(q, i):
        j, h = units[q][i]
        a, layer = chunks[j]
        cut = pl.ds(h * half[a], half[a])
        mine = pl.ds(pl.multiple_of(me * rows[a] + h * half[a], STRIP), half[a])
        t = i % SETS
        return [
            pltpu.make_async_copy(m[a].at[layer, cut], m_set[q].at[t], set_in.at[q, t, 0]),
            pltpu.make_async_copy(v[a].at[layer, cut], v_set[q].at[t], set_in.at[q, t, 1]),
            pltpu.make_async_copy(w[a].at[layer, mine], w_set[q].at[t], set_in.at[q, t, 2]),
        ], [
            pltpu.make_async_copy(m_set[q].at[t], m_out[a].at[layer, cut], set_out.at[q, t, 0]),
            pltpu.make_async_copy(v_set[q].at[t], v_out[a].at[layer, cut], set_out.at[q, t, 1]),
        ]

    def start_set(q, i):
        if i < len(units[q]):
            if i >= SETS:
                for copy in set_copies(q, i - SETS)[1]:
                    copy.wait()
            for copy in set_copies(q, i)[0]:
                copy.start()

    for q in range(shapes):
        for i in range(SETS - 1):
            start_set(q, i)

    def update(j, h, extra):
        a, _ = chunks[j]
        q = kinds[a]
        i = units[q].index((j, h))
        ins, outs = set_copies(q, i)
        for copy in ins:
            copy.wait()
        mm, vv, ww = (s[q].at[i % SETS] for s in (m_set, v_set, w_set))

        def finish(strip, grad):
            old = f32(ww[strip, :])
            new_m = 0.9 * mm[strip, :] + 0.1 * grad
            new_v = 0.95 * vv[strip, :] + 0.05 * grad * grad
            mm[strip, :] = new_m
            vv[strip, :] = new_v
            step = new_m * lax.rsqrt(new_v + 1e-8) + 0.1 * old
            return (old - 0.02 * step).astype(jnp.bfloat16)

        do(add_own(j, 0, h, extra, finish))
        for copy in outs:
            copy.start()
        start_set(q, i + SETS - 1)

    def block(a, layer, chip_of, core_of, h=None, start=0, end=None):
        base = (chip_of * CORES + core_of) * rows[a] + (0 if h is None else h * half[a]) + start
        size = (rows[a] if h is None else half[a]) if end is None else end
        return w_out[a].at[layer, pl.ds(pl.multiple_of(base, STRIP), size - start)]

    def gather_copy(j, n):
        a, layer = chunks[j]
        s = (gather_send.at[j, n], gather_recv.at[j, n])
        mine = lambda h: part[a].at[layer, 0, pl.ds(h * half[a], half[a])]
        if n < 4:
            h, to = n % 2, right if n < 2 else left
            return remote(mine(h), block(a, layer, chip, core, h), *s, to)
        if n < 6:
            d, h, to = ((chips - 1, 0, right), (1, 1, left))[n - 4]
            skip = LAST if j == gathered[-1] else 0
            there = block(a, layer, turn[d], core, h, skip)
            return remote(there, far_half[h].at[layer, pl.ds(skip, half[a] - skip)] if a == last - 1 else there, *s, to)
        if n == 6:
            return remote(part[a].at[layer, 0], block(a, layer, chip, core), *s, partner)
        d, h = ((chips - 1, None), (1, None), (far, 0), (far, 1))[n - 7]
        there = block(a, layer, turn[d], core, h)
        return remote(there, there, *s, partner)

    def go(j, n):
        finish_later(gather_copy(j, n), "wait_send", *(("wait_recv",) if n >= 6 else ()))

    def final(j):
        a, layer = chunks[j]
        if a == last:
            for h, slots in enumerate(((2, 4), (1, 5))):
                update(j, h, [arrival(j, slot) for slot in slots])
                half_of = part[a].at[layer, 0, pl.ds(h * half[a], half[a])]
                finish_later(pltpu.make_async_copy(half_of, new_half[h].at[layer], local_sem.at[j, h]), "wait")
            pair = remote(part[a].at[layer, 0], new_pair.at[layer], gather_send.at[j, 6], gather_recv.at[j, 6], partner)
            finish_later(pair, "wait_send", "wait_recv")
            return
        update(j, 0, (arrival(j, 2), arrival(j, 4)))
        go(j, 0)
        update(j, 1, (arrival(j, 1), arrival(j, 5)))
        go(j, 3)
        go(j, 1)
        go(j, 2)
        go(j, 6)
        finish_later(pltpu.make_async_copy(part[a].at[layer, 0], block(a, layer, chip, core), local_sem.at[j, 0]), "wait")

    def pass_on(j):
        a, layer = chunks[j]
        for n, then, d, h in ((0, 4, chips - 1, 0), (3, 5, 1, 1)):
            gather_copy(j, n).wait_recv()
            go(j, then)
            if j == gathered[-1]:
                finish_later(pltpu.make_async_copy(block(a, layer, turn[d], core, h, 0, LAST), to_pass[h].at[0], pass_sem.at[h]), "wait")
        gather_copy(j, 1).wait_recv()
        go(j, 7)
        gather_copy(j, 2).wait_recv()
        go(j, 8)

    def hand_over(j):
        for n, then in ((4, 9), (5, 10)):
            gather_copy(j, n).wait_recv()
            if chunks[j][0] != last - 1:
                go(j, then)

    pl.semaphore_wait(barrier, 3)

    acts = {"pair": start_pair, "follow": follow, "lead": lead, "first": first, "middle": middle, "final": final, "pass": pass_on, "hand": hand_over}
    for act, j in plan:
        acts[act](j)

    for q in range(shapes):
        for i in range(max(0, len(units[q]) - SETS), len(units[q])):
            for copy in set_copies(q, i)[1]:
                copy.wait()
    for wait in waits:
        wait()


def relayed(targets, pieces, near=(), leave=VMEM * 3 // 4):
    near = {id(x) for x in near}
    arrays = list({id(p[1]): p[1] for p in pieces}.values())
    at = {id(x): n for n, x in enumerate(arrays)}
    intos = [(n, t) for n, t in enumerate(targets) if not isinstance(t, jax.ShapeDtypeStruct)]
    through, direct = ([p for p in pieces if (id(p[1]) in near) == one] for one in (False, True))

    def body(*refs):
        take = iter(refs[len(intos) :])
        srcs, dsts, bufs = ([next(take) for _ in one] for one in (arrays, targets, through))
        sems = next(take)
        me = lax.axis_index("dp")
        place = me // CORES, me % CORES
        ins, outs = [], []
        for n, (t, x, _, here, there) in enumerate(through):
            ins.append(pltpu.make_async_copy(srcs[at[id(x)]].at[here(*place)], bufs[n], sems.at[n, 0]))
            outs.append(pltpu.make_async_copy(bufs[n], dsts[t].at[there(*place)], sems.at[n, 1]))
        for copy in ins:
            copy.start()
        for n, (t, x, _, here, there) in enumerate(direct):
            copy = pltpu.make_async_copy(srcs[at[id(x)]].at[here(*place)], dsts[t].at[there(*place)], sems.at[len(through) + n, 1])
            copy.start()
            outs.append(copy)
        for come, go in zip(ins, outs, strict=False):
            come.wait()
            go.start()
        for copy in outs:
            copy.wait()

    any_space = pl.BlockSpec(memory_space=pltpu.HBM)
    return pl.pallas_call(
        body,
        out_shape=[jax.ShapeDtypeStruct(t.shape, t.dtype) for t in targets],
        in_specs=[any_space] * len(intos) + [pl.BlockSpec(memory_space=pltpu.VMEM) if id(x) in near else any_space for x in arrays],
        out_specs=[any_space] * len(targets),
        scratch_shapes=[pltpu.VMEM(shape, x.dtype) for _, x, shape, *_ in through] + [pltpu.SemaphoreType.DMA((len(pieces), 2))],
        input_output_aliases={i: n for i, (n, _) in enumerate(intos)},
        compiler_params=pltpu.CompilerParams(vmem_limit_bytes=VMEM - leave),
    )(*[t for _, t in intos], *arrays)


def moved(arrays, steps, hole):
    def body(*refs):
        for src, dst in zip(refs[: len(arrays)], refs[len(arrays) :], strict=True):
            dst[...] = src[...]

    def spec(n, x):
        def at(i, j):
            if n != hole[0]:
                return i, j, 0
            step = jnp.where(j == hole[1], j - 1, j)
            return i, lax.rem(lax.axis_index("dp") // CORES + step, steps[1]), 0

        return pl.BlockSpec((x.shape[0] // steps[0], x.shape[1] // steps[1], x.shape[2]), at)

    specs = [spec(n, x) for n, x in enumerate(arrays)]
    return pl.pallas_call(
        body,
        out_shape=[jax.ShapeDtypeStruct(x.shape, x.dtype) for x in arrays],
        grid=steps,
        in_specs=specs,
        out_specs=specs,
        compiler_params=pltpu.CompilerParams(vmem_limit_bytes=VMEM),
    )(*arrays)


def placed(chips, targets, blocks, **options):
    def piece(t, x, d, other, first):
        rows = targets[t].shape[1] // (chips * CORES)

        def there(chip, core):
            base = (lax.rem(chip + d, chips) * CORES + (1 - core if other else core)) * rows + first
            layers = targets[t].shape[0]
            return (pl.ds(layers - x.shape[0], x.shape[0]), pl.ds(pl.multiple_of(base, STRIP), x.shape[1]))

        return (t, x, x.shape, lambda chip, core: slice(None), there)

    return relayed(targets, [piece(*one) for one in blocks], **options)


def solution(mesh):
    devices = mesh.shape["dp"]
    chips = devices // CORES

    def hop(x, d):
        return lax.ppermute(x, "dp", [(i, (i + d * CORES) % devices) for i in range(devices)])

    def across(x):
        return lax.ppermute(x, "dp", [(i, i // CORES * CORES + 1 - i % CORES) for i in range(devices)])

    def step(*arrays):
        terms, weights, m, v = (arrays[i : i + 3] for i in (0, 3, 6, 9))
        count, layers = len(weights), weights[0].shape[0]
        blocks = [one.shape[1:] for one in m]
        distinct = list(dict.fromkeys(blocks))
        kinds = tuple(distinct.index(b) for b in blocks)
        chunks = count * layers
        any_space = pl.BlockSpec(memory_space=pl.ANY)
        bf16 = jnp.bfloat16
        halves = [(b[0] // 2, b[1]) for b in distinct]
        cut_rows = blocks[-1][0] // 2
        dma = pltpu.SemaphoreType.DMA
        cut_cols, (far_rows, far_cols) = blocks[-1][1], (blocks[-2][0] // 2, blocks[-2][1])
        tail = [(layers, cut_rows, cut_cols)] * 2 + [(layers, *blocks[-1])] + [(layers, far_rows, far_cols)] * 2 + [(1, LAST, far_cols)] * 2
        early = (2, blocks[0][0] // 2 // STRIP)
        out = pl.pallas_call(
            functools.partial(kernel, chips, layers, kinds),
            out_shape=[jax.ShapeDtypeStruct(one.shape, one.dtype) for one in weights[:-1]]
            + [jax.ShapeDtypeStruct(one, bf16) for one in tail]
            + [jax.ShapeDtypeStruct(one.shape, one.dtype) for one in (*m, *v)],
            in_specs=[any_space] * 4 * count,
            out_specs=[any_space] * (3 * count - 1 + len(tail)),
            scratch_shapes=[pltpu.VMEM((layers, chips, *b), bf16) for b in blocks]
            + [pltpu.VMEM((layers, 6, b[0] // 2, b[1]), bf16) for b in blocks]
            + [pltpu.VMEM((SLOTS, *b), bf16) for b in halves]
            + [pltpu.VMEM((SETS, *b), jnp.float32) for b in halves] * 2
            + [pltpu.VMEM((SETS, *b), bf16) for b in halves]
            + [dma((len(distinct), SLOTS)), dma((len(distinct), SETS, 3)), dma((len(distinct), SETS, 2))]
            + [dma((chunks * 2 * chips,))] * 2
            + [dma((chunks * 6,))] * 2
            + [dma((chunks, 11))] * 2
            + [dma((chunks, 2))]
            + [dma(early)] * 4
            + [pltpu.SemaphoreType.REGULAR, dma((2,))],
            compiler_params=pltpu.CompilerParams(collective_id=0, has_side_effects=True, vmem_limit_bytes=VMEM),
        )(*terms, *weights, *m, *v)
        new, (own_a, own_b, pair, late_a, late_b, last_a, last_b), moments = out[: count - 1], out[count - 1 : count - 1 + len(tail)], out[count - 1 + len(tail) :]
        far, hold = chips // 2, lax.optimization_barrier
        back, down = chips - 1, cut_rows
        put = functools.partial(placed, chips)
        left_a, right_b = hop(own_a, 1), hop(own_b, -1)
        left_b, right_a = hop(own_b, 1), hop(own_a, -1)
        results = list(moved([*new, *moments], (layers, chips), (count - 2, far)))
        left_a, right_b, late_a, late_b, last_a, last_b, results = hold((left_a, right_b, late_a, late_b, last_a, last_b, results))
        far_a, far_b = hop(left_a, 1), hop(right_b, -1)
        last_a, last_b = hop(last_a, 1), hop(last_b, -1)
        over = [across(x) for x in (left_a, right_b, left_b, right_a)]
        over_late = across(late_a), across(late_b)
        held = sum(x.size * x.dtype.itemsize for x in (*over, *over_late, far_a, far_b, last_a, last_b)) + 2**18
        near = [(0, own_a, 0, 0, 0), (0, own_b, 0, 0, down), (0, pair, 0, 1, 0), (0, left_a, back, 0, 0), (0, right_b, 1, 0, down)]
        near += [(0, left_b, back, 0, down), (0, right_a, 1, 0, 0), (1, late_a, far, 0, 0), (1, late_b, far, 0, far_rows)]
        whole, results[count - 2] = put([jax.ShapeDtypeStruct(weights[-1].shape, bf16), results[count - 2]], near, leave=held)
        over, over_late, whole, results = hold((over, over_late, whole, results))
        near = [(0, over[0], back, 1, 0), (0, over[1], 1, 1, down), (0, over[2], back, 1, down), (0, over[3], 1, 1, 0)]
        near += [(1, over_late[0], far, 1, 0), (1, over_late[1], far, 1, far_rows)]
        whole, results[count - 2] = put([whole, results[count - 2]], near, near=[*over, *over_late])
        far_a, whole = hold((far_a, whole))
        over_far_a = across(far_a)
        far_b, whole = hold((far_b, whole))
        over_far_b = across(far_b)
        [whole] = put([whole], [(0, far_a, far, 0, 0), (0, far_b, far, 0, down)], near=[far_a, far_b])
        last_a, last_b, whole = hold((last_a, last_b, whole))
        over_last_a, over_last_b = across(last_a), across(last_b)
        over_far_a, whole = hold((over_far_a, whole))
        some = [(0, over_far_a, far, 1, 0), (1, last_a, far, 0, 0), (1, last_b, far, 0, far_rows)]
        whole, results[count - 2] = put([whole, results[count - 2]], some, near=[over_far_a, last_a, last_b])
        over_far_b, over_last_a, over_last_b, whole, results = hold((over_far_b, over_last_a, over_last_b, whole, results))
        some = [(0, over_far_b, far, 1, down), (1, over_last_a, far, 1, 0), (1, over_last_b, far, 1, far_rows)]
        whole, results[count - 2] = put([whole, results[count - 2]], some, near=[over_far_b, over_last_a, over_last_b])
        return (*results[: count - 1], whole, *results[count - 1 :])

    all_of, cut = P(None, None, None), P(None, "dp", None)
    return jax.shard_map(
        step,
        mesh=mesh,
        in_specs=(P(("rep", "dp"), None, None, None),) * 3 + (all_of,) * 3 + (cut,) * 6,
        out_specs=(P("rep", None, None),) * 3 + (P("rep", "dp", None),) * 6,
        check_vma=False,
    )
```
